256 devices in a mesh: gz: 64 (over x, z, core), gy: 4 (over y).
Axes of the slice: x: 4, y: 4, z: 8, core: 2. Of those that a mesh axis runs over, the one named last changes fastest.
Arguments:
- source_first: float32 [512, 32, 16, 128], P('gz', 'gy'), may hold values from -6 to 6
- source_second: float32 [256, 16, 16, 128], P('gz', 'gy'), may hold values from -6 to 6
- source_third: float32 [128, 8, 16, 128], P('gz', 'gy'), may hold values from -6 to 6
- source_fourth: float32 [64, 4, 16, 128], P('gz', 'gy'), may hold values from -6 to 6
- guess_first: float32 [512, 32, 16, 128], P('gz', 'gy'), may hold values from -6 to 6
- guess_second: float32 [256, 16, 16, 128], P('gz', 'gy'), may hold values from -6 to 6
- guess_third: float32 [128, 8, 16, 128], P('gz', 'gy'), may hold values from -6 to 6
- guess_fourth: float32 [64, 4, 16, 128], P('gz', 'gy'), may hold values from -6 to 6
- shift_first: float32 [512, 32, 128], P('gz', 'gy'), may hold values from 0.2 to 2
- shift_second: float32 [256, 16, 128], P('gz', 'gy'), may hold values from 0.2 to 2
- shift_third: float32 [128, 8, 128], P('gz', 'gy'), may hold values from 0.2 to 2
- shift_fourth: float32 [64, 4, 128], P('gz', 'gy'), may hold values from 0.2 to 2
- blocks_first: bfloat16 [512, 32, 2, 128, 128], P('gz', 'gy'), may hold values from -0.375 to 0.375
- blocks_second: bfloat16 [256, 16, 2, 128, 128], P('gz', 'gy'), may hold values from -0.375 to 0.375
- blocks_third: bfloat16 [128, 8, 2, 128, 128], P('gz', 'gy'), may hold values from -0.375 to 0.375
- links_first: int32 [512, 32, 2], P('gz', 'gy'), may hold values from 0 to 4095, as said below
- links_second: int32 [256, 16, 2], P('gz', 'gy'), may hold values from 0 to 1023, as said below
- links_third: int32 [128, 8, 2], P('gz', 'gy'), may hold values from 0 to 255, as said below
Outputs:
- smooth_first: float32 [512, 32, 16, 128], P('gz', 'gy')
- smooth_second: float32 [256, 16, 16, 128], P('gz', 'gy')
- smooth_third: float32 [128, 8, 16, 128], P('gz', 'gy')
- smooth_fourth: float32 [64, 4, 16, 128], P('gz', 'gy')
The draws below stay inside these ranges and needn't reach their ends.
Inputs may be any that keep to these rules, and one draw needn't show every extreme that they name: `links_first`: entry k of fine cell (i, j) names coarse column x * 16 + y with x within one of i // 2 and y within one of j // 2, both periodic on the coarse grid. `links_second`: entry k of cell (i, j) names coarse column x * 8 + y with x within one of i // 2 and y within one of j // 2, both periodic on the coarse grid. `links_third`: entry k of cell (i, j) names coarse column x * 4 + y with x within one of i // 2 and y within one of j // 2, both periodic on the coarse grid.
All inputs are finite; a program needn't handle non-finite values.
Results may differ from the reference program's by a relative error of at most 0.0005.
Values may be sent and summed in bfloat16 or wider, within the bound.
A program may use at most 256 MiB of HBM per device.

```python
import math
import jax
import jax.numpy as jnp
from jax import lax

LINE = 128
SIDES = 16
LINKS = 2
DEGREE = 3
NX0 = 512
NY0 = 32
NX1 = 256
NY1 = 16
NX2 = 128
NY2 = 8
NX3 = 64
NY3 = 4


def column_links(key, fine_rows, fine_cols, coarse_rows, coarse_cols):
    offsets = jax.random.randint(jax.random.fold_in(key, 17), (fine_rows, fine_cols, LINKS, 2), -1, 2)
    row_index = (jnp.arange(fine_rows, dtype=jnp.int32) // 2)[:, None, None]
    col_index = (jnp.arange(fine_cols, dtype=jnp.int32) // 2)[None, :, None]
    coarse_row = (row_index + offsets[..., 0]) % coarse_rows
    coarse_col = (col_index + offsets[..., 1]) % coarse_cols
    return (coarse_row * coarse_cols + coarse_col).astype(jnp.int32)


def draw_links_first(key, part):
    return column_links(key, NX0, NY0, NX1, NY1)


def draw_links_second(key, part):
    return column_links(key, NX1, NY1, NX2, NY2)


def draw_links_third(key, part):
    return column_links(key, NX2, NY2, NX3, NY3)


def level_of(own_key, extent, shards, low, high):
    loudness = 1.0
    for position, shards_of in shards:
        draws = jax.random.uniform(jax.random.fold_in(jax.random.fold_in(own_key, 6), position), (shards_of,), jnp.float32, low / len(shards), high / len(shards))
        loudness = loudness * jnp.repeat(jnp.exp(draws), extent[position] // shards_of).reshape((-1,) + (1,) * (len(extent) - 1 - position))
    return loudness


def centred(key, shape, width, most, shards=(), held_as=jnp.bfloat16):
    factor_of = level_of(key, shape, shards, -0.22, 0.18) if shards else 1.0
    array = jax.random.normal(key, shape, jnp.float32) * width * factor_of
    return jnp.minimum(jnp.maximum(array, -most), most).astype(held_as)


def setup_inputs(seed: int = 0) -> dict:
    key_list = jax.random.split(jax.random.key(seed), 19)
    source_first = centred(key_list[0], (NX0, NY0, SIDES, LINE), 1.0, 6.0, ((0, 64), (1, 4)), jnp.float32)
    source_second = centred(key_list[1], (NX1, NY1, SIDES, LINE), 1.0, 6.0, ((0, 64), (1, 4)), jnp.float32)
    source_third = centred(key_list[2], (NX2, NY2, SIDES, LINE), 1.0, 6.0, ((0, 64), (1, 4)), jnp.float32)
    source_fourth = centred(key_list[3], (NX3, NY3, SIDES, LINE), 1.0, 6.0, ((0, 64), (1, 4)), jnp.float32)
    guess_first = centred(key_list[4], (NX0, NY0, SIDES, LINE), 1.0, 6.0, ((0, 64), (1, 4)), jnp.float32)
    guess_second = centred(key_list[5], (NX1, NY1, SIDES, LINE), 1.0, 6.0, ((0, 64), (1, 4)), jnp.float32)
    guess_third = centred(key_list[6], (NX2, NY2, SIDES, LINE), 1.0, 6.0, ((0, 64), (1, 4)), jnp.float32)
    guess_fourth = centred(key_list[7], (NX3, NY3, SIDES, LINE), 1.0, 6.0, ((0, 64), (1, 4)), jnp.float32)
    shift_first = jnp.clip(jnp.exp(math.log(2.0) - 2.3025851 * jax.random.uniform(key_list[8], (NX0, NY0, LINE), jnp.float32) ** level_of(key_list[8], (NX0, NY0, LINE), ((0, 64), (1, 4)), -0.2, 0.2)), 0.2, 2.0)
    shift_second = jnp.clip(jnp.exp(math.log(2.0) - 2.3025851 * jax.random.uniform(key_list[9], (NX1, NY1, LINE), jnp.float32) ** level_of(key_list[9], (NX1, NY1, LINE), ((0, 64), (1, 4)), -0.2, 0.2)), 0.2, 2.0)
    shift_third = jnp.clip(jnp.exp(math.log(2.0) - 2.3025851 * jax.random.uniform(key_list[10], (NX2, NY2, LINE), jnp.float32) ** level_of(key_list[10], (NX2, NY2, LINE), ((0, 64), (1, 4)), -0.2, 0.2)), 0.2, 2.0)
    shift_fourth = jnp.clip(jnp.exp(math.log(2.0) - 2.3025851 * jax.random.uniform(key_list[11], (NX3, NY3, LINE), jnp.float32) ** level_of(key_list[11], (NX3, NY3, LINE), ((0, 64), (1, 4)), -0.2, 0.2)), 0.2, 2.0)
    blocks_first = centred(key_list[12], (NX0, NY0, LINKS, LINE, LINE), (LINKS * LINE) ** -0.5, 0.375, ((0, 64), (1, 4)))
    blocks_second = centred(key_list[13], (NX1, NY1, LINKS, LINE, LINE), (LINKS * LINE) ** -0.5, 0.375, ((0, 64), (1, 4)))
    blocks_third = centred(key_list[14], (NX2, NY2, LINKS, LINE, LINE), (LINKS * LINE) ** -0.5, 0.375, ((0, 64), (1, 4)))
    links_first = draw_links_first(jax.random.fold_in(key_list[18], 71), 0)
    links_second = draw_links_second(jax.random.fold_in(key_list[18], 71), 0)
    links_third = draw_links_third(jax.random.fold_in(key_list[18], 71), 0)
    return {"source_first": source_first, "source_second": source_second, "source_third": source_third, "source_fourth": source_fourth, "guess_first": guess_first, "guess_second": guess_second, "guess_third": guess_third, "guess_fourth": guess_fourth, "shift_first": shift_first, "shift_second": shift_second, "shift_third": shift_third, "shift_fourth": shift_fourth, "blocks_first": blocks_first, "blocks_second": blocks_second, "blocks_third": blocks_third, "links_first": links_first, "links_second": links_second, "links_third": links_third}


upper_edge = 14.0
lower_edge = upper_edge / 8.0


def operate(vector, diagonal):
    beside = jnp.roll(vector, 1, 0) + jnp.roll(vector, -1, 0)
    beside = beside + jnp.roll(vector, 1, 1) + jnp.roll(vector, -1, 1)
    beside = beside + jnp.roll(vector, 1, 3) + jnp.roll(vector, -1, 3)
    return (6.0 + diagonal[:, :, None, :]) * vector - beside


def chebyshev(source, initial, diagonal):
    centre = (upper_edge + lower_edge) / 2.0
    half_width = (upper_edge - lower_edge) / 2.0
    ratio_edge = centre / half_width
    factor = 1.0 / ratio_edge
    residual = source - operate(initial, diagonal)
    direction = residual / centre
    result = initial
    for sweep_index in range(DEGREE):
        result = result + direction
        if sweep_index + 1 < DEGREE:
            residual = residual - operate(direction, diagonal)
            factor_next = 1.0 / (2.0 * ratio_edge - factor)
            direction = factor_next * factor * direction + (2.0 * factor_next / half_width) * residual
            factor = factor_next
    return result


def prolong(coarse, link_ids, blocks):
    coarse_lines = coarse.astype(jnp.bfloat16).reshape((-1,) + coarse.shape[2:])

    def one_row(row_pair):
        row_links, row_blocks = row_pair
        picked = coarse_lines[row_links].astype(jnp.float32)
        return jnp.einsum("bkrj,bkij->bri", picked, row_blocks.astype(jnp.float32),
                          precision=lax.Precision.HIGHEST)

    return lax.map(one_row, (link_ids, blocks))


def reference(source_first, source_second, source_third, source_fourth,
              guess_first, guess_second, guess_third, guess_fourth,
              shift_first, shift_second, shift_third, shift_fourth,
              blocks_first, blocks_second, blocks_third,
              links_first, links_second, links_third):
    smooth_fourth = chebyshev(source_fourth, guess_fourth, shift_fourth)
    start_third = guess_third + prolong(smooth_fourth, links_third, blocks_third)
    smooth_third = chebyshev(source_third, start_third, shift_third)
    start_second = guess_second + prolong(smooth_third, links_second, blocks_second)
    smooth_second = chebyshev(source_second, start_second, shift_second)
    start_first = guess_first + prolong(smooth_second, links_first, blocks_first)
    smooth_first = chebyshev(source_first, start_first, shift_first)
    return (smooth_first, smooth_second, smooth_third, smooth_fourth)
```

```python
import functools

import jax
import jax.numpy as jnp
from jax import lax
from jax.experimental import pallas as pl
from jax.experimental.pallas import tpu as pltpu
from jax.sharding import PartitionSpec as P

MESH = pl.DeviceIdType.MESH

upper_edge = 14.0
lower_edge = upper_edge / 8.0
CENTRE = (upper_edge + lower_edge) / 2.0
HALF = (upper_edge - lower_edge) / 2.0
RATIO = CENTRE / HALF
FACTOR_0 = 1.0 / RATIO
FACTOR_1 = 1.0 / (2.0 * RATIO - FACTOR_0)
FACTOR_2 = 1.0 / (2.0 * RATIO - FACTOR_1)
A2, B2 = FACTOR_1 * FACTOR_0, 2.0 * FACTOR_1 / HALF
A3, B3 = FACTOR_2 * FACTOR_1, 2.0 * FACTOR_2 / HALF

RADIUS = 3
RINGS = (0, 0, 0, 0)


class Level:
    def __init__(self, nz, ny, peers_z, peers_y, ring):
        self.nz, self.ny, self.ring = nz, ny, ring
        self.peers_y = peers_y
        self.halo = RADIUS + ring
        self.total_y = ny * peers_y
        self.full = ny + 2 * self.halo >= self.total_y
        self.rows = nz + 2 * self.halo
        self.cols = self.total_y if self.full else ny + 2 * self.halo
        self.off = 0 if self.full else self.halo

    def col(self, y):
        return y % self.total_y if self.full else y + self.off

    def needed(self, z, y, radius):
        def gap(p, n):
            return max(0, -p - self.ring, p - (n - 1) - self.ring)

        turns = (-1, 0, 1) if self.full else (0,)
        gap_y = min(gap(y + t * self.total_y, self.ny) for t in turns)
        return gap(z, self.nz) + gap_y <= radius

    def messages(self, radius):
        found = []
        reach = -(-self.halo // self.nz)
        offsets_y = range(-(self.peers_y // 2 - 1), self.peers_y // 2 + 1) if self.full else range(-1, 2)
        for oz in range(-reach, reach + 1):
            for oy in offsets_y:
                if (oz, oy) == (0, 0):
                    continue
                spans = []
                for i in range(self.nz):
                    js = [j for j in range(self.ny) if self.needed(i - oz * self.nz, j - oy * self.ny, radius)]
                    if not js:
                        continue
                    span = (js[0], len(js))
                    if spans and spans[-1][1] == span:
                        spans[-1][2] += 1
                    else:
                        spans.append([i, span, 1])
                for i, (j, count), rows in spans:
                    found.append((oz, oy, i, j, rows, count))
        return found


def ring_messages(nz, ny):
    found = []
    for oz in (-1, 0, 1):
        for oy in (-1, 0, 1):
            if (oz, oy) == (0, 0):
                continue
            i, rows = (0, nz) if oz == 0 else ((nz - 1, 1) if oz == 1 else (0, 1))
            j, count = (0, ny) if oy == 0 else ((ny - 1, 1) if oy == 1 else (0, 1))
            found.append((oz, oy, i, j, rows, count))
    return found


def plan(shapes, peers_z, peers_y):
    levels = [Level(nz, ny, peers_z, peers_y, ring) for (nz, ny), ring in zip(shapes, RINGS)]
    table = []
    for number, level in enumerate(levels):
        for kind, radius in (("u", RADIUS), ("f", RADIUS - 1), ("t", RADIUS - 1)):
            table += [(kind, number, m) for m in level.messages(radius)]
        if number < len(levels) - 1 and level.ring == 0:
            table += [("c", number, m) for m in ring_messages(level.nz, level.ny)]
    return levels, table


def rolls(v):
    return pltpu.roll(v, 1, 1) + pltpu.roll(v, v.shape[1] - 1, 1)


def kernel(levels, table, peers, *refs):
    n = len(levels)
    source, guess, shift = refs[0:n], refs[n : 2 * n], refs[2 * n : 3 * n]
    refs = refs[3 * n :]
    blocks, links = (None,) + refs[: n - 1], (None,) + refs[n - 1 : 2 * n - 2]
    refs = refs[2 * n - 2 :]
    outs, refs = refs[:n], refs[n:]
    u, f, t, d1, d2 = (refs[k * n : (k + 1) * n] for k in range(5))
    refs = refs[5 * n :]
    g, b, c = (None,) + refs[: n - 1], (None,) + refs[n - 1 : 2 * n - 2], refs[2 * n - 2 : 3 * n - 3]
    result = refs[3 * n - 3 : 4 * n - 3]
    local_sem, out_sem, send_sem, recv_sem = refs[4 * n - 3 :]

    peers_z, peers_y = peers
    my_z, my_y = lax.axis_index("gz"), lax.axis_index("gy")

    def peer(oz, oy):
        return (lax.rem(my_z + (oz + peers_z), peers_z), lax.rem(my_y + (oy + peers_y), peers_y))

    barrier = pltpu.get_barrier_semaphore()
    partners = sorted({m[:2] for _, _, m in table})
    for oz, oy in partners:
        pl.semaphore_signal(barrier, inc=1, device_id=peer(oz, oy), device_id_type=MESH)

    loads = {}

    def load(key, src, dst):
        loads[key] = pltpu.make_async_copy(src, dst, local_sem.at[len(loads)])
        loads[key].start()

    for number, level in enumerate(levels):
        own = (pl.ds(level.halo, level.nz), pl.ds(level.off, level.ny))
        load(("f", number), source[number], f[number].at[own])
        load(("t", number), shift[number], t[number].at[own])
        if number == 0:
            load(("g", 0), guess[0], u[0].at[own])
    for number in range(1, n):
        load(("g", number), guess[number], g[number])
        load(("b", number), blocks[number], b[number])

    buffers = {"u": u, "f": f, "t": t, "c": c}
    copies = {}

    def describe(index):
        kind, number, (oz, oy, i, j, rows, count) = table[index]
        level, ref = levels[number], buffers[kind][number]
        zi, yj = i - oz * level.nz, j - oy * level.ny
        if kind == "c":
            source_at = (pl.ds(1 + i, rows), pl.ds(1 + j, count))
            target_at = (pl.ds(1 + zi, rows), pl.ds(1 + yj, count))
        else:
            source_at = (pl.ds(level.halo + i, rows), pl.ds(level.col(j), count))
            target_at = (pl.ds(level.halo + zi, rows), pl.ds(level.col(yj), count))
        return pltpu.make_async_remote_copy(
            src_ref=ref.at[source_at],
            dst_ref=ref.at[target_at],
            send_sem=send_sem.at[index],
            recv_sem=recv_sem.at[index],
            device_id=peer(oz, oy),
            device_id_type=MESH,
        )

    def send(kind, number):
        for index, (k, l, _) in enumerate(table):
            if (k, l) == (kind, number):
                copies[index] = describe(index)
                copies[index].start()

    def receive(kind, number):
        for index, (k, l, _) in enumerate(table):
            if (k, l) == (kind, number):
                copies[index].wait_recv()

    def sweep(level, ring, body):
        def row(z, carry):
            if level.full:
                cells = range(level.cols)
            else:
                cells = range(level.off - ring, level.off + level.ny + ring)
            for y in cells:
                body(z, y)
            return carry

        lax.fori_loop(level.halo - ring, level.halo + level.nz + ring, row, 0)

    def beside(level, ref, z, y, middle):
        up, down = ((y + 1) % level.cols, (y - 1) % level.cols) if level.full else (y + 1, y - 1)
        return ref[z - 1, y] + ref[z + 1, y] + ref[z, up] + ref[z, down] + rolls(middle)

    def smooth(number):
        level = levels[number]
        uu, ff, tt, p, q = u[number], f[number], t[number], d1[number], d2[number]
        ring = level.ring

        def first(z, y):
            v = uu[z, y]
            p[z, y] = (ff[z, y] - ((6.0 + tt[z, y]) * v - beside(level, uu, z, y, v))) * (1.0 / CENTRE)

        def second(z, y):
            v = p[z, y]
            q[z, y] = ((A2 + B2 * CENTRE) - B2 * (6.0 + tt[z, y])) * v + B2 * beside(level, p, z, y, v)

        def third(z, y):
            v, w = q[z, y], p[z, y]
            out = uu[z, y] + (1.0 - B3 * A2 / B2) * w
            out = out + ((1.0 + A3 + B3 / B2) - B3 * (6.0 + tt[z, y])) * v + B3 * beside(level, q, z, y, v)
            finish(z, y, out)

        def finish(z, y, out):
            at = y - level.off
            if 0 <= at < level.ny:
                if ring == 0:
                    result[number][z - level.halo, at] = out
                    if number < n - 1:
                        c[number][z - level.halo + 1, at + 1] = out.astype(jnp.bfloat16)
                else:
                    result[number][z - level.halo + ring, at] = out
            if ring:
                for turn in (0, level.total_y if level.full else 0):
                    col = at + 1 - turn
                    if 0 <= col < level.ny + 2:
                        c[number][z - level.halo + 1, col] = out.astype(jnp.bfloat16)
                        break

        sweep(level, ring + 2, first)
        sweep(level, ring + 1, second)
        if level.full:
            wanted = sorted({y % level.total_y for y in range(-ring, level.ny + ring)})
        else:
            wanted = range(level.off - ring, level.off + level.ny + ring)

        def row(z, carry):
            for y in wanted:
                third(z, y)
            return carry

        lax.fori_loop(level.halo - ring, level.halo + level.nz + ring, row, 0)
        own = result[number] if ring == 0 else result[number].at[pl.ds(ring, level.nz)]
        out_copy = pltpu.make_async_copy(own, outs[number], out_sem.at[number])
        out_copy.start()
        return out_copy

    def prolong(number):
        level, coarse = levels[number], levels[number - 1]
        full_cols = coarse.ny * peers_y
        full_rows = coarse.nz * peers_z
        base_row = my_z * coarse.nz - 1
        base_col = my_y * coarse.ny - 1

        def row(i, carry):
            for j in range(level.ny):
                total = g[number][i, j]
                for k in range(2):
                    link = links[number][(i, j, k) if level.ny == 2 else (i, k, j)]
                    at_row = lax.rem(link // full_cols - base_row + full_rows, full_rows)
                    at_col = lax.rem(lax.rem(link, full_cols) - base_col + full_cols, full_cols)
                    total = total + lax.dot_general(
                        c[number - 1][jnp.minimum(at_row, coarse.nz + 1), jnp.minimum(at_col, coarse.ny + 1)],
                        b[number][i, j, k],
                        (((1,), (1,)), ((), ())),
                        preferred_element_type=jnp.float32,
                    )
                u[number][level.halo + i, level.off + j] = total
            return carry

        lax.fori_loop(0, level.nz, row, 0)

    for key in (("f", 0), ("t", 0), ("g", 0)):
        loads[key].wait()
    pl.semaphore_wait(barrier, len(partners))
    for kind in ("u", "f", "t"):
        send(kind, 0)
    for number in range(1, n):
        for kind in ("f", "t"):
            loads[(kind, number)].wait()
            send(kind, number)
    outputs = []
    for number in range(n):
        if number:
            loads[("g", number)].wait()
            loads[("b", number)].wait()
            prolong(number)
            send("u", number)
        for kind in ("f", "t", "u"):
            receive(kind, number)
        outputs.append(smooth(number))
        if number < n - 1 and levels[number].ring == 0:
            send("c", number)
            receive("c", number)
    for index in range(len(table)):
        copies[index].wait_send()
    for copy in outputs:
        copy.wait()


def shards(peers, *arrays):
    fine_to_coarse = lambda group: group[::-1]
    source, guess, shift = (fine_to_coarse(arrays[k : k + 4]) for k in (0, 4, 8))
    blocks, links = (fine_to_coarse(arrays[k : k + 3]) for k in (12, 15))
    n = len(source)
    sides, line = source[0].shape[2:]
    levels, table = plan([x.shape[:2] for x in source], *peers)
    shift = [x.reshape(x.shape[0], x.shape[1], 1, line) for x in shift]
    links = [x if x.shape[1] == x.shape[2] else x.transpose(0, 2, 1) for x in links]
    f32, bf16 = jnp.float32, jnp.bfloat16
    extended = [pltpu.VMEM((l.rows, l.cols, sides, line), f32) for l in levels]
    scratch = extended + extended + [pltpu.VMEM((l.rows, l.cols, 1, line), f32) for l in levels] + extended + extended
    scratch += [pltpu.VMEM(x.shape, f32) for x in guess[1:]]
    scratch += [pltpu.VMEM(x.shape, bf16) for x in blocks]
    scratch += [pltpu.VMEM((l.nz + 2, l.ny + 2, sides, line), bf16) for l in levels[:-1]]
    scratch += [pltpu.VMEM((l.nz + 2 * l.ring, l.ny, sides, line), f32) for l in levels]
    scratch += [
        pltpu.SemaphoreType.DMA((3 * n + 2 * (n - 1),)),
        pltpu.SemaphoreType.DMA((n,)),
        pltpu.SemaphoreType.DMA((len(table),)),
        pltpu.SemaphoreType.DMA((len(table),)),
    ]
    hbm = pl.BlockSpec(memory_space=pltpu.HBM)
    results = pl.pallas_call(
        functools.partial(kernel, levels, table, peers),
        out_shape=[jax.ShapeDtypeStruct(x.shape, f32) for x in source],
        in_specs=[hbm] * (3 * n + len(blocks)) + [pl.BlockSpec(memory_space=pltpu.SMEM)] * len(links),
        out_specs=[hbm] * n,
        scratch_shapes=scratch,
        compiler_params=pltpu.CompilerParams(
            collective_id=0, has_side_effects=True, vmem_limit_bytes=67043328
        ),
    )(*source, *guess, *shift, *blocks, *links)
    return tuple(results[::-1])


def solution(mesh):
    wide = P("gz", "gy", None, None)
    flat = P("gz", "gy", None)
    in_specs = (wide,) * 8 + (flat,) * 4 + (P("gz", "gy", None, None, None),) * 3 + (flat,) * 3
    peers = (mesh.shape["gz"], mesh.shape["gy"])
    return jax.shard_map(
        functools.partial(shards, peers), mesh=mesh, in_specs=in_specs, out_specs=(wide,) * 4, check_vma=False
    )
```

```python
import functools

import jax
import jax.numpy as jnp
from jax import lax
from jax.experimental import pallas as pl
from jax.experimental.pallas import tpu as pltpu
from jax.sharding import PartitionSpec as P

MESH = pl.DeviceIdType.MESH

upper_edge = 14.0
lower_edge = upper_edge / 8.0
CENTRE = (upper_edge + lower_edge) / 2.0
HALF = (upper_edge - lower_edge) / 2.0
RATIO = CENTRE / HALF
FACTOR_0 = 1.0 / RATIO
FACTOR_1 = 1.0 / (2.0 * RATIO - FACTOR_0)
FACTOR_2 = 1.0 / (2.0 * RATIO - FACTOR_1)
A2, B2 = FACTOR_1 * FACTOR_0, 2.0 * FACTOR_1 / HALF
A3, B3 = FACTOR_2 * FACTOR_1, 2.0 * FACTOR_2 / HALF

RADIUS = 3
RINGS = (0, 0, 0, 0)
STRAIGHT = 40
ROWS = 2


class Level:
    def __init__(self, nz, ny, peers_z, peers_y, ring):
        self.nz, self.ny, self.ring = nz, ny, ring
        self.peers_y = peers_y
        self.halo = RADIUS + ring
        self.total_y = ny * peers_y
        self.full = ny + 2 * self.halo >= self.total_y
        self.rows = nz + 2 * self.halo
        self.cols = self.total_y if self.full else ny + 2 * self.halo
        self.off = 0 if self.full else self.halo
        self.cols_of_ring = sorted({self.col(y) for y in range(-ring, ny + ring)})

    def col(self, y):
        return y % self.total_y if self.full else y + self.off

    def needed(self, z, y, radius):
        def gap(p, n):
            return max(0, -p - self.ring, p - (n - 1) - self.ring)

        turns = (-1, 0, 1) if self.full else (0,)
        gap_y = min(gap(y + t * self.total_y, self.ny) for t in turns)
        return gap(z, self.nz) + gap_y <= radius

    def messages(self, radius):
        found = []
        reach = -(-self.halo // self.nz)
        offsets_y = range(-(self.peers_y // 2 - 1), self.peers_y // 2 + 1) if self.full else range(-1, 2)
        for oz in range(-reach, reach + 1):
            for oy in offsets_y:
                if (oz, oy) == (0, 0):
                    continue
                spans = []
                for i in range(self.nz):
                    js = [j for j in range(self.ny) if self.needed(i - oz * self.nz, j - oy * self.ny, radius)]
                    if not js:
                        continue
                    span = (js[0], len(js))
                    if spans and spans[-1][1] == span:
                        spans[-1][2] += 1
                    else:
                        spans.append([i, span, 1])
                for i, (j, count), rows in spans:
                    found.append((oz, oy, i, j, rows, count))
        return found


def ring_messages(nz, ny):
    found = []
    for oz in (-1, 0, 1):
        for oy in (-1, 0, 1):
            if (oz, oy) == (0, 0):
                continue
            i, rows = (0, nz) if oz == 0 else ((nz - 1, 1) if oz == 1 else (0, 1))
            j, count = (0, ny) if oy == 0 else ((ny - 1, 1) if oy == 1 else (0, 1))
            found.append((oz, oy, i, j, rows, count))
    return found


def plan(shapes, peers_z, peers_y):
    levels = [Level(nz, ny, peers_z, peers_y, ring) for (nz, ny), ring in zip(shapes, RINGS)]
    table = []
    for number, level in enumerate(levels):
        for kind, radius in (("u", RADIUS), ("f", RADIUS - 1), ("t", RADIUS - 1)):
            table += [(kind, number, m) for m in level.messages(radius)]
        if number < len(levels) - 1 and level.ring == 0:
            table += [("c", number, m) for m in ring_messages(level.nz, level.ny)]
    return levels, table


def modulo(value, size):
    return (value + size) & (size - 1) if size & (size - 1) == 0 else lax.rem(value + size, size)


def rolls(v):
    return pltpu.roll(v, 1, 1) + pltpu.roll(v, v.shape[1] - 1, 1)


def kernel(levels, table, peers, *refs):
    n = len(levels)
    source, guess, shift = refs[0:n], refs[n : 2 * n], refs[2 * n : 3 * n]
    refs = refs[3 * n :]
    blocks, links = (None,) + refs[: n - 1], (None,) + refs[n - 1 : 2 * n - 2]
    refs = refs[2 * n - 2 :]
    outs, refs = refs[:n], refs[n:]
    u, f, t, d1, d2 = (refs[k * n : (k + 1) * n] for k in range(5))
    refs = refs[5 * n :]
    g, b, c = (None,) + refs[: n - 1], (None,) + refs[n - 1 : 2 * n - 2], refs[2 * n - 2 : 3 * n - 3]
    result = refs[3 * n - 3 : 4 * n - 3]
    lines, refs = (None,) + refs[4 * n - 3 : 5 * n - 4], refs[5 * n - 4 :]
    local_sem, out_sem, send_sem, recv_sem = refs
    c_flat = [x.reshape((-1,) + x.shape[2:]) for x in c]

    peers_z, peers_y = peers
    my_z, my_y = lax.axis_index("gz"), lax.axis_index("gy")

    def peer(oz, oy):
        return (lax.rem(my_z + (oz + peers_z), peers_z), lax.rem(my_y + (oy + peers_y), peers_y))

    barrier = pltpu.get_barrier_semaphore()
    partners = sorted({m[:2] for _, _, m in table})
    for oz, oy in partners:
        pl.semaphore_signal(barrier, inc=1, device_id=peer(oz, oy), device_id_type=MESH)

    loads = {}

    def load(key, src, dst):
        loads[key] = pltpu.make_async_copy(src, dst, local_sem.at[len(loads)])
        loads[key].start()

    for number, level in enumerate(levels):
        own = (pl.ds(level.halo, level.nz), pl.ds(level.off, level.ny))
        load(("f", number), source[number], f[number].at[own])
        load(("t", number), shift[number], t[number].at[own])
        if number == 0:
            load(("g", 0), guess[0], u[0].at[own])
    for number in range(1, n):
        load(("g", number), guess[number], g[number])
        load(("b", number), blocks[number], b[number])

    buffers = {"u": u, "f": f, "t": t, "c": c}
    copies = {}

    def describe(index):
        kind, number, (oz, oy, i, j, rows, count) = table[index]
        level, ref = levels[number], buffers[kind][number]
        zi, yj = i - oz * level.nz, j - oy * level.ny
        if kind == "c":
            source_at = (pl.ds(1 + i, rows), pl.ds(1 + j, count))
            target_at = (pl.ds(1 + zi, rows), pl.ds(1 + yj, count))
        else:
            source_at = (pl.ds(level.halo + i, rows), pl.ds(level.col(j), count))
            target_at = (pl.ds(level.halo + zi, rows), pl.ds(level.col(yj), count))
        return pltpu.make_async_remote_copy(
            src_ref=ref.at[source_at],
            dst_ref=ref.at[target_at],
            send_sem=send_sem.at[index],
            recv_sem=recv_sem.at[index],
            device_id=peer(oz, oy),
            device_id_type=MESH,
        )

    def send(kind, number):
        for index, (k, l, _) in enumerate(table):
            if (k, l) == (kind, number):
                copies[index] = describe(index)
                copies[index].start()

    def receive(kind, number):
        for index, (k, l, _) in enumerate(table):
            if (k, l) == (kind, number):
                copies[index].wait_recv()

    def sweep(level, ring, body, after=None):
        cols = sorted({level.col(y) for y in range(-ring, level.ny + ring)})
        first, count = level.halo - ring, level.nz + 2 * ring
        step = count if count * len(cols) <= STRAIGHT else ROWS

        def rows(start):
            for z in range(step):
                for y in cols:
                    body(start + z, y)
            if after is not None:
                after(start, step)

        if step == count:
            rows(first)
        else:
            lax.fori_loop(0, count // step, lambda i, carry: (rows(first + i * step), carry)[1], 0)

    def beside(level, ref, z, y, middle):
        up, down = ((y + 1) % level.cols, (y - 1) % level.cols) if level.full else (y + 1, y - 1)
        return ref[z - 1, y] + ref[z + 1, y] + ref[z, up] + ref[z, down] + rolls(middle)

    def smooth(number):
        level = levels[number]
        uu, ff, tt, p, q = u[number], f[number], t[number], d1[number], d2[number]
        ring = level.ring

        def first(z, y):
            v = uu[z, y]
            p[z, y] = (ff[z, y] - ((6.0 + tt[z, y]) * v - beside(level, uu, z, y, v))) * (1.0 / CENTRE)

        def second(z, y):
            v = p[z, y]
            q[z, y] = ((A2 + B2 * CENTRE) - B2 * (6.0 + tt[z, y])) * v + B2 * beside(level, p, z, y, v)

        def third(z, y):
            v, w = q[z, y], p[z, y]
            out = uu[z, y] + (1.0 - B3 * A2 / B2) * w
            out = out + ((1.0 + A3 + B3 / B2) - B3 * (6.0 + tt[z, y])) * v + B3 * beside(level, q, z, y, v)
            finish(z, y, out)

        def finish(z, y, out):
            result[number][z - level.halo + ring, level.cols_of_ring.index(y)] = out
            if number < n - 1:
                at = (y - level.off + 1) % level.total_y if level.full else y - level.off + 1
                c[number][z - level.halo + 1, at] = out.astype(jnp.bfloat16)

        def copy_out(start, rows):
            at = start - level.halo
            own = result[number].at[pl.ds(at, rows)]
            pltpu.make_async_copy(own, outs[number].at[pl.ds(at, rows)], out_sem.at[number]).start()

        sweep(level, ring + 2, first)
        sweep(level, ring + 1, second)
        sweep(level, ring, third, None if ring else copy_out)
        own = result[number]
        if ring:
            own_cols = level.cols_of_ring.index(level.off)
            own = own.at[pl.ds(ring, level.nz), pl.ds(own_cols, level.ny)]
            pltpu.make_async_copy(own, outs[number], out_sem.at[number]).start()
        return pltpu.make_async_copy(own, outs[number], out_sem.at[number])

    def index_lines(number):
        level, coarse = levels[number], levels[number - 1]
        base_row = my_z * coarse.nz - 1
        base_col = my_y * coarse.ny - 1

        def row(i, carry):
            for j in range(level.ny):
                for k in range(2):
                    link = links[number][(i, j, k) if level.ny == 2 else (i, k, j)]
                    at_row = modulo(link // coarse.total_y - base_row, coarse.nz * peers_z)
                    at_col = modulo(link - base_col, coarse.total_y)
                    at = jnp.minimum(at_row, coarse.nz + 1) * (coarse.ny + 2) + jnp.minimum(at_col, coarse.ny + 1)
                    lines[number][(i * level.ny + j) * 2 + k] = at
            return carry

        lax.fori_loop(0, level.nz, row, 0)

    def prolong(number):
        level = levels[number]

        def row(i, carry):
            for j in range(level.ny):
                at = (i * level.ny + j) * 2
                picked = [c_flat[number - 1][lines[number][at + k]] for k in range(2)]
                total = g[number][i, j] + lax.dot_general(
                    jnp.concatenate(picked, axis=1),
                    jnp.concatenate([b[number][i, j, 0], b[number][i, j, 1]], axis=1),
                    (((1,), (1,)), ((), ())),
                    preferred_element_type=jnp.float32,
                )
                u[number][level.halo + i, level.off + j] = total
            return carry

        lax.fori_loop(0, level.nz, row, 0)

    for number in range(1, n):
        index_lines(number)
    for key in (("f", 0), ("t", 0), ("g", 0)):
        loads[key].wait()
    pl.semaphore_wait(barrier, len(partners))
    for kind in ("u", "f", "t"):
        send(kind, 0)
    for number in range(1, n):
        for kind in ("f", "t"):
            loads[(kind, number)].wait()
            send(kind, number)
    outputs = []
    for number in range(n):
        if number:
            loads[("g", number)].wait()
            loads[("b", number)].wait()
            prolong(number)
            send("u", number)
        for kind in ("f", "t", "u"):
            receive(kind, number)
        outputs.append(smooth(number))
        if number < n - 1 and levels[number].ring == 0:
            send("c", number)
            receive("c", number)
    for index in range(len(table)):
        copies[index].wait_send()
    for copy in outputs:
        copy.wait()


def shards(peers, *arrays):
    fine_to_coarse = lambda group: group[::-1]
    source, guess, shift = (fine_to_coarse(arrays[k : k + 4]) for k in (0, 4, 8))
    blocks, links = (fine_to_coarse(arrays[k : k + 3]) for k in (12, 15))
    n = len(source)
    sides, line = source[0].shape[2:]
    levels, table = plan([x.shape[:2] for x in source], *peers)
    shift = [x.reshape(x.shape[0], x.shape[1], 1, line) for x in shift]
    links = [x if x.shape[1] == x.shape[2] else x.transpose(0, 2, 1) for x in links]
    f32, bf16 = jnp.float32, jnp.bfloat16
    extended = [pltpu.VMEM((l.rows, l.cols, sides, line), f32) for l in levels]
    scratch = extended + extended + [pltpu.VMEM((l.rows, l.cols, 1, line), f32) for l in levels] + extended + extended
    scratch += [pltpu.VMEM(x.shape, f32) for x in guess[1:]]
    scratch += [pltpu.VMEM(x.shape, bf16) for x in blocks]
    scratch += [pltpu.VMEM((l.nz + 2, l.ny + 2, sides, line), bf16) for l in levels[:-1]]
    scratch += [pltpu.VMEM((l.nz + 2 * l.ring, len(l.cols_of_ring), sides, line), f32) for l in levels]
    scratch += [pltpu.SMEM((2 * l.nz * l.ny,), jnp.int32) for l in levels[1:]]
    scratch += [
        pltpu.SemaphoreType.DMA((3 * n + 2 * (n - 1),)),
        pltpu.SemaphoreType.DMA((n,)),
        pltpu.SemaphoreType.DMA((len(table),)),
        pltpu.SemaphoreType.DMA((len(table),)),
    ]
    hbm = pl.BlockSpec(memory_space=pltpu.HBM)
    results = pl.pallas_call(
        functools.partial(kernel, levels, table, peers),
        out_shape=[jax.ShapeDtypeStruct(x.shape, f32) for x in source],
        in_specs=[hbm] * (3 * n + len(blocks)) + [pl.BlockSpec(memory_space=pltpu.SMEM)] * len(links),
        out_specs=[hbm] * n,
        scratch_shapes=scratch,
        compiler_params=pltpu.CompilerParams(
            collective_id=0, has_side_effects=True, vmem_limit_bytes=67043328
        ),
    )(*source, *guess, *shift, *blocks, *links)
    return tuple(results[::-1])


def solution(mesh):
    wide = P("gz", "gy", None, None)
    flat = P("gz", "gy", None)
    in_specs = (wide,) * 8 + (flat,) * 4 + (P("gz", "gy", None, None, None),) * 3 + (flat,) * 3
    peers = (mesh.shape["gz"], mesh.shape["gy"])
    return jax.shard_map(
        functools.partial(shards, peers), mesh=mesh, in_specs=in_specs, out_specs=(wide,) * 4, check_vma=False
    )
```

```python
import functools

import jax
import jax.numpy as jnp
from jax import lax
from jax.experimental import pallas as pl
from jax.experimental.pallas import tpu as pltpu
from jax.sharding import PartitionSpec as P

MESH = pl.DeviceIdType.MESH

upper_edge = 14.0
lower_edge = upper_edge / 8.0
CENTRE = (upper_edge + lower_edge) / 2.0
HALF = (upper_edge - lower_edge) / 2.0
RATIO = CENTRE / HALF
FACTOR_0 = 1.0 / RATIO
FACTOR_1 = 1.0 / (2.0 * RATIO - FACTOR_0)
FACTOR_2 = 1.0 / (2.0 * RATIO - FACTOR_1)
A2, B2 = FACTOR_1 * FACTOR_0, 2.0 * FACTOR_1 / HALF
A3, B3 = FACTOR_2 * FACTOR_1, 2.0 * FACTOR_2 / HALF

RADIUS = 3
RINGS = (0, 1, 0, 0)
STRAIGHT = 64
PIECE = 4
ROWS = 5


class Level:
    def __init__(self, nz, ny, peers_z, peers_y, ring):
        self.nz, self.ny, self.ring = nz, ny, ring
        self.peers_y = peers_y
        self.halo = RADIUS + ring
        self.total_y = ny * peers_y
        self.full = ny + 2 * self.halo >= self.total_y
        self.rows = nz + 2 * self.halo
        self.cols = self.total_y if self.full else ny + 2 * self.halo
        self.off = 0 if self.full else self.halo

    def col(self, y):
        return y % self.total_y if self.full else y + self.off

    def needed(self, z, y, radius):
        def gap(p, n):
            return max(0, -p - self.ring, p - (n - 1) - self.ring)

        turns = (-1, 0, 1) if self.full else (0,)
        gap_y = min(gap(y + t * self.total_y, self.ny) for t in turns)
        return gap(z, self.nz) + gap_y <= radius

    def messages(self, radius):
        found = []
        reach = -(-self.halo // self.nz)
        offsets_y = range(-(self.peers_y // 2 - 1), self.peers_y // 2 + 1) if self.full else range(-1, 2)
        for oz in range(-reach, reach + 1):
            for oy in offsets_y:
                if (oz, oy) == (0, 0):
                    continue
                spans = []
                for i in range(self.nz):
                    js = [j for j in range(self.ny) if self.needed(i - oz * self.nz, j - oy * self.ny, radius)]
                    if not js:
                        continue
                    span = (js[0], len(js))
                    if spans and spans[-1][1] == span:
                        spans[-1][2] += 1
                    else:
                        spans.append([i, span, 1])
                for i, (j, count), rows in spans:
                    for part in range(i, i + rows, PIECE):
                        found.append((oz, oy, part, j, min(PIECE, i + rows - part), count))
        return sorted(found, key=lambda m: -abs(m[1]))


def ring_messages(nz, ny):
    found = []
    for oz in (-1, 0, 1):
        for oy in (-1, 0, 1):
            if (oz, oy) == (0, 0):
                continue
            i, rows = (0, nz) if oz == 0 else ((nz - 1, 1) if oz == 1 else (0, 1))
            j, count = (0, ny) if oy == 0 else ((ny - 1, 1) if oy == 1 else (0, 1))
            found.append((oz, oy, i, j, rows, count))
    return found


def plan(shapes, peers_z, peers_y):
    levels = [Level(nz, ny, peers_z, peers_y, ring) for (nz, ny), ring in zip(shapes, RINGS)]
    table = []
    for number, level in enumerate(levels):
        for kind, radius in (("u", RADIUS), ("f", RADIUS - 1), ("t", RADIUS - 1)):
            table += [(kind, number, m) for m in level.messages(radius)]
        if number < len(levels) - 1 and level.ring == 0:
            table += [("c", number, m) for m in ring_messages(level.nz, level.ny)]
    return levels, table


def modulo(value, size):
    return (value + size) & (size - 1) if size & (size - 1) == 0 else lax.rem(value + size, size)


def rolls(v):
    return pltpu.roll(v, 1, 1) + pltpu.roll(v, v.shape[1] - 1, 1)


def kernel(levels, table, peers, *refs):
    n = len(levels)
    source, guess, shift = refs[0:n], refs[n : 2 * n], refs[2 * n : 3 * n]
    refs = refs[3 * n :]
    blocks, links = (None,) + refs[: n - 1], (None,) + refs[n - 1 : 2 * n - 2]
    refs = refs[2 * n - 2 :]
    outs, refs = refs[:n], refs[n:]
    u, f, t, d1, d2 = (refs[k * n : (k + 1) * n] for k in range(5))
    refs = refs[5 * n :]
    g, b, c = (None,) + refs[: n - 1], (None,) + refs[n - 1 : 2 * n - 2], refs[2 * n - 2 : 3 * n - 3]
    lines, link_lines = (None,) + refs[3 * n - 3 : 4 * n - 4], (None,) + refs[4 * n - 4 : 5 * n - 5]
    local_sem, send_sem, recv_sem = refs[5 * n - 5 :]
    c_flat = [x.reshape((-1,) + x.shape[2:]) for x in c]

    peers_z, peers_y = peers
    my_z, my_y = lax.axis_index("gz"), lax.axis_index("gy")

    def peer(oz, oy):
        return (lax.rem(my_z + (oz + peers_z), peers_z), lax.rem(my_y + (oy + peers_y), peers_y))

    barrier = pltpu.get_barrier_semaphore()
    partners = sorted({m[:2] for _, _, m in table})
    for oz, oy in partners:
        pl.semaphore_signal(barrier, inc=1, device_id=peer(oz, oy), device_id_type=MESH)

    loads = {}

    def load(key, src, dst):
        loads[key] = pltpu.make_async_copy(src, dst, local_sem.at[len(loads)])
        loads[key].start()

    for number, level in enumerate(levels):
        own = (pl.ds(level.halo, level.nz), pl.ds(level.off, level.ny))
        load(("f", number), source[number], f[number].at[own])
        load(("t", number), shift[number], t[number].at[own])
        if number == 0:
            load(("g", 0), guess[0], u[0].at[own])
    for number in range(1, n):
        load(("l", number), links[number], link_lines[number])
        load(("g", number), guess[number], g[number])
        load(("b", number), blocks[number], b[number])

    buffers = {"u": u, "f": f, "t": t, "c": c}
    copies = {}

    def describe(index):
        kind, number, (oz, oy, i, j, rows, count) = table[index]
        level, ref = levels[number], buffers[kind][number]
        zi, yj = i - oz * level.nz, j - oy * level.ny
        if kind == "c":
            source_at = (pl.ds(1 + i, rows), pl.ds(1 + j, count))
            target_at = (pl.ds(1 + zi, rows), pl.ds(1 + yj, count))
        else:
            source_at = (pl.ds(level.halo + i, rows), pl.ds(level.col(j), count))
            target_at = (pl.ds(level.halo + zi, rows), pl.ds(level.col(yj), count))
        return pltpu.make_async_remote_copy(
            src_ref=ref.at[source_at],
            dst_ref=ref.at[target_at],
            send_sem=send_sem.at[index],
            recv_sem=recv_sem.at[index],
            device_id=peer(oz, oy),
            device_id_type=MESH,
        )

    def send(kind, number, end=None):
        for index, (k, l, m) in enumerate(table):
            if (k, l) == (kind, number) and (end is None or m[2] + m[4] == end):
                copies[index] = describe(index)
                copies[index].start()

    def receive(kind, number):
        for index, (k, l, _) in enumerate(table):
            if (k, l) == (kind, number):
                copies[index].wait_recv()

    def sweep(level, ring, body, after=None):
        cols = sorted({level.col(y) for y in range(-ring, level.ny + ring)})
        first, count = level.halo - ring, level.nz + 2 * ring
        step = count if count * len(cols) <= STRAIGHT else max(k for k in range(1, ROWS + 1) if count % k == 0)

        def rows(start):
            for z in range(step):
                for y in cols:
                    body(start + z, y)
            if after is not None:
                after(start, step)

        if step == count:
            rows(first)
        else:
            lax.fori_loop(0, count // step, lambda i, carry: (rows(first + i * step), carry)[1], 0)

    def beside(level, ref, z, y, middle):
        up, down = ((y + 1) % level.cols, (y - 1) % level.cols) if level.full else (y + 1, y - 1)
        return ref[z - 1, y] + ref[z + 1, y] + ref[z, up] + ref[z, down] + rolls(middle)

    def smooth(number):
        level = levels[number]
        uu, ff, tt, p, q = u[number], f[number], t[number], d1[number], d2[number]
        ring = level.ring

        def first(z, y):
            v = uu[z, y]
            p[z, y] = (ff[z, y] - ((6.0 + tt[z, y]) * v - beside(level, uu, z, y, v))) * (1.0 / CENTRE)

        def second(z, y):
            v = p[z, y]
            q[z, y] = ((A2 + B2 * CENTRE) - B2 * (6.0 + tt[z, y])) * v + B2 * beside(level, p, z, y, v)

        def third(z, y):
            v, w = q[z, y], p[z, y]
            out = uu[z, y] + (1.0 - B3 * A2 / B2) * w
            out = out + ((1.0 + A3 + B3 / B2) - B3 * (6.0 + tt[z, y])) * v + B3 * beside(level, q, z, y, v)
            finish(z, y, out)

        def finish(z, y, out):
            row, col = z - level.halo, y - level.off
            if ring == 0 or (0 <= row < level.nz and 0 <= col < level.ny):
                outs[number][row, col] = out
            if number < n - 1:
                at = (col + 1) % level.total_y if level.full else col + 1
                c[number][row + 1, at] = out.astype(jnp.bfloat16)

        sweep(level, ring + 2, first)
        sweep(level, ring + 1, second)
        sweep(level, ring, third)

    def index_lines(number):
        level, coarse = levels[number], levels[number - 1]
        base_row = my_z * coarse.nz - 1
        base_col = my_y * coarse.ny - 1

        def row(i, carry):
            for j in range(level.ny):
                for k in range(2):
                    link = link_lines[number][(i, j, k) if level.ny == 2 else (i, k, j)]
                    at_row = modulo(link // coarse.total_y - base_row, coarse.nz * peers_z)
                    at_col = modulo(link - base_col, coarse.total_y)
                    at = jnp.minimum(at_row, coarse.nz + 1) * (coarse.ny + 2) + jnp.minimum(at_col, coarse.ny + 1)
                    lines[number][(i * level.ny + j) * 2 + k] = at
            return carry

        lax.fori_loop(0, level.nz, row, 0)

    def prolong(number):
        level = levels[number]

        def row(i, carry):
            for j in range(level.ny):
                at = (i * level.ny + j) * 2
                picked = [c_flat[number - 1][lines[number][at + k]] for k in range(2)]
                total = g[number][i, j] + lax.dot_general(
                    jnp.concatenate(picked, axis=1),
                    jnp.concatenate([b[number][i, j, 0], b[number][i, j, 1]], axis=1),
                    (((1,), (1,)), ((), ())),
                    preferred_element_type=jnp.float32,
                )
                u[number][level.halo + i, level.off + j] = total
            return carry

        ends = sorted({m[2] + m[4] for k, l, m in table if (k, l) == ("u", number)} | {level.nz})
        start = 0
        for end in ends:
            lax.fori_loop(start, end, row, 0)
            send("u", number, end)
            start = end

    for number in range(1, n):
        loads[("l", number)].wait()
        index_lines(number)
    for key in (("f", 0), ("t", 0), ("g", 0)):
        loads[key].wait()
    pl.semaphore_wait(barrier, len(partners))
    def send_inputs(number):
        for kind in ("t", "f"):
            loads[(kind, number)].wait()
            send(kind, number)

    for kind in ("u", "f", "t"):
        send(kind, 0)
    send_inputs(1)
    for number in range(n):
        if number:
            loads[("g", number)].wait()
            loads[("b", number)].wait()
            prolong(number)
            if number == 1:
                send_inputs(3)
        for kind in ("f", "t", "u"):
            receive(kind, number)
        smooth(number)
        send("c", number)
        if number == 0:
            send_inputs(2)
        receive("c", number)
    for index in range(len(table)):
        copies[index].wait_send()


def copy_out(*refs):
    results, outs, sem = refs[: len(refs) // 2], refs[len(refs) // 2 : -1], refs[-1]
    copies = [pltpu.make_async_copy(r, o, sem.at[k]) for k, (r, o) in enumerate(zip(results, outs))]
    for copy in copies:
        copy.start()
    for copy in copies:
        copy.wait()


def shards(peers, *arrays):
    fine_to_coarse = lambda group: group[::-1]
    source, guess, shift = (fine_to_coarse(arrays[k : k + 4]) for k in (0, 4, 8))
    blocks, links = (fine_to_coarse(arrays[k : k + 3]) for k in (12, 15))
    n = len(source)
    sides, line = source[0].shape[2:]
    levels, table = plan([x.shape[:2] for x in source], *peers)
    shift = [x.reshape(x.shape[0], x.shape[1], 1, line) for x in shift]
    links = [x if x.shape[1] == x.shape[2] else x.transpose(0, 2, 1) for x in links]
    f32, bf16 = jnp.float32, jnp.bfloat16
    extended = [pltpu.VMEM((l.rows, l.cols, sides, line), f32) for l in levels]
    scratch = extended + extended + [pltpu.VMEM((l.rows, l.cols, 1, line), f32) for l in levels] + extended + extended
    scratch += [pltpu.VMEM(x.shape, f32) for x in guess[1:]]
    scratch += [pltpu.VMEM(x.shape, bf16) for x in blocks]
    scratch += [pltpu.VMEM((l.nz + 2, l.ny + 2, sides, line), bf16) for l in levels[:-1]]
    scratch += [pltpu.SMEM((2 * l.nz * l.ny,), jnp.int32) for l in levels[1:]]
    scratch += [pltpu.SMEM(x.shape, jnp.int32) for x in links]
    scratch += [
        pltpu.SemaphoreType.DMA((3 * n + 3 * (n - 1),)),
        pltpu.SemaphoreType.DMA((len(table),)),
        pltpu.SemaphoreType.DMA((len(table),)),
    ]
    hbm, vmem = pl.BlockSpec(memory_space=pltpu.HBM), pl.BlockSpec(memory_space=pltpu.VMEM)
    operands = [pltpu.with_memory_space_constraint(x, pltpu.HBM) for x in (*source, *guess, *shift, *blocks, *links)]
    shapes = [jax.ShapeDtypeStruct(x.shape, f32) for x in source]
    results = pl.pallas_call(
        functools.partial(kernel, levels, table, peers),
        out_shape=shapes,
        in_specs=[hbm] * len(operands),
        out_specs=[vmem] * n,
        scratch_shapes=scratch,
        compiler_params=pltpu.CompilerParams(
            collective_id=0, has_side_effects=True, vmem_limit_bytes=32 * 1024 * 1024
        ),
    )(*operands)
    results = pl.pallas_call(
        copy_out,
        out_shape=shapes,
        in_specs=[pl.BlockSpec(memory_space=pl.ANY)] * n,
        out_specs=[hbm] * n,
        scratch_shapes=[pltpu.SemaphoreType.DMA((n,))],
        compiler_params=pltpu.CompilerParams(vmem_limit_bytes=2 * 1024 * 1024),
    )(*results)
    return tuple(results[::-1])


def solution(mesh):
    wide = P("gz", "gy", None, None)
    flat = P("gz", "gy", None)
    in_specs = (wide,) * 8 + (flat,) * 4 + (P("gz", "gy", None, None, None),) * 3 + (flat,) * 3
    peers = (mesh.shape["gz"], mesh.shape["gy"])
    return jax.shard_map(
        functools.partial(shards, peers), mesh=mesh, in_specs=in_specs, out_specs=(wide,) * 4, check_vma=False
    )
```

```python
import functools

import jax
import jax.numpy as jnp
from jax import lax
from jax.experimental import pallas as pl
from jax.experimental.pallas import tpu as pltpu
from jax.sharding import PartitionSpec as P

MESH = pl.DeviceIdType.MESH

upper_edge = 14.0
lower_edge = upper_edge / 8.0
CENTRE = (upper_edge + lower_edge) / 2.0
HALF = (upper_edge - lower_edge) / 2.0
RATIO = CENTRE / HALF
FACTOR_0 = 1.0 / RATIO
FACTOR_1 = 1.0 / (2.0 * RATIO - FACTOR_0)
FACTOR_2 = 1.0 / (2.0 * RATIO - FACTOR_1)
A2, B2 = FACTOR_1 * FACTOR_0, 2.0 * FACTOR_1 / HALF
A3, B3 = FACTOR_2 * FACTOR_1, 2.0 * FACTOR_2 / HALF

RADIUS = 3
RINGS = (0, 1, 0, 0)
STRAIGHT = 64
PROLONG_ROWS = 2
PIECE = 4
ROWS = 5


class Level:
    def __init__(self, nz, ny, peers_z, peers_y, ring):
        self.nz, self.ny, self.ring = nz, ny, ring
        self.peers_y = peers_y
        self.halo = RADIUS + ring
        self.total_y = ny * peers_y
        self.full = ny + 2 * self.halo >= self.total_y
        self.rows = nz + 2 * self.halo
        self.cols = self.total_y if self.full else ny + 2 * self.halo
        self.off = 0 if self.full else self.halo

    def col(self, y):
        return y % self.total_y if self.full else y + self.off

    def needed(self, z, y, radius):
        def gap(p, n):
            return max(0, -p - self.ring, p - (n - 1) - self.ring)

        turns = (-1, 0, 1) if self.full else (0,)
        gap_y = min(gap(y + t * self.total_y, self.ny) for t in turns)
        return gap(z, self.nz) + gap_y <= radius

    def messages(self, radius):
        found = []
        reach = -(-self.halo // self.nz)
        offsets_y = range(-(self.peers_y // 2 - 1), self.peers_y // 2 + 1) if self.full else range(-1, 2)
        for oz in range(-reach, reach + 1):
            for oy in offsets_y:
                if (oz, oy) == (0, 0):
                    continue
                spans = []
                for i in range(self.nz):
                    js = [j for j in range(self.ny) if self.needed(i - oz * self.nz, j - oy * self.ny, radius)]
                    if not js:
                        continue
                    span = (js[0], len(js))
                    if spans and spans[-1][1] == span:
                        spans[-1][2] += 1
                    else:
                        spans.append([i, span, 1])
                for i, (j, count), rows in spans:
                    for part in range(i, i + rows, PIECE):
                        found.append((oz, oy, part, j, min(PIECE, i + rows - part), count))
        return sorted(found, key=lambda m: -abs(m[1]))


def ring_messages(nz, ny):
    found = []
    for oz in (-1, 0, 1):
        for oy in (-1, 0, 1):
            if (oz, oy) == (0, 0):
                continue
            i, rows = (0, nz) if oz == 0 else ((nz - 1, 1) if oz == 1 else (0, 1))
            j, count = (0, ny) if oy == 0 else ((ny - 1, 1) if oy == 1 else (0, 1))
            found.append((oz, oy, i, j, rows, count))
    return found


def plan(shapes, peers_z, peers_y):
    levels = [Level(nz, ny, peers_z, peers_y, ring) for (nz, ny), ring in zip(shapes, RINGS)]
    table = []
    for number, level in enumerate(levels):
        for kind, radius in (("u", RADIUS), ("f", RADIUS - 1), ("t", RADIUS - 1)):
            table += [(kind, number, m) for m in level.messages(radius)]
        if number < len(levels) - 1 and level.ring == 0:
            table += [("c", number, m) for m in ring_messages(level.nz, level.ny)]
    return levels, table


def groups_of(table):
    return sorted({(kind, number) for kind, number, _ in table})


def group_lines(table, group):
    lines = {"u": 16, "f": 16, "t": 1, "c": 8}[group[0]]
    return sum(lines * m[4] * m[5] for kind, number, m in table if (kind, number) == group)


def modulo(value, size):
    return (value + size) & (size - 1) if size & (size - 1) == 0 else lax.rem(value + size, size)


def rolls(v):
    return pltpu.roll(v, 1, 1) + pltpu.roll(v, v.shape[1] - 1, 1)


def kernel(levels, table, peers, *refs):
    n = len(levels)
    source, guess, shift = refs[0:n], refs[n : 2 * n], refs[2 * n : 3 * n]
    refs = refs[3 * n :]
    blocks, links = (None,) + refs[: n - 1], (None,) + refs[n - 1 : 2 * n - 2]
    refs = refs[2 * n - 2 :]
    outs, refs = refs[:n], refs[n:]
    u, f, t, d1, d2 = (refs[k * n : (k + 1) * n] for k in range(5))
    refs = refs[5 * n :]
    g, b, c = (None,) + refs[: n - 1], (None,) + refs[n - 1 : 2 * n - 2], refs[2 * n - 2 : 3 * n - 3]
    lines, link_lines = (None,) + refs[3 * n - 3 : 4 * n - 4], (None,) + refs[4 * n - 4 : 5 * n - 5]
    sizer, local_sem, send_sem, recv_sem = refs[5 * n - 5 :]
    c_flat = [x.reshape((-1,) + x.shape[2:]) for x in c]

    peers_z, peers_y = peers
    my_z, my_y = lax.axis_index("gz"), lax.axis_index("gy")

    def peer(oz, oy):
        return (lax.rem(my_z + (oz + peers_z), peers_z), lax.rem(my_y + (oy + peers_y), peers_y))

    barrier = pltpu.get_barrier_semaphore()
    partners = sorted({m[:2] for _, _, m in table})
    for oz, oy in partners:
        pl.semaphore_signal(barrier, inc=1, device_id=peer(oz, oy), device_id_type=MESH)

    loads = {}

    def load(key, src, dst):
        loads[key] = pltpu.make_async_copy(src, dst, local_sem.at[len(loads)])
        loads[key].start()

    for number, level in enumerate(levels):
        own = (pl.ds(level.halo, level.nz), pl.ds(level.off, level.ny))
        load(("f", number), source[number], f[number].at[own])
        load(("t", number), shift[number], t[number].at[own])
        if number == 0:
            load(("g", 0), guess[0], u[0].at[own])
    for number in range(1, n):
        load(("l", number), links[number], link_lines[number])
        load(("g", number), guess[number], g[number])
        load(("b", number), blocks[number], b[number])

    buffers = {"u": u, "f": f, "t": t, "c": c}
    groups = groups_of(table)

    def describe(index):
        kind, number, (oz, oy, i, j, rows, count) = table[index]
        level, ref = levels[number], buffers[kind][number]
        zi, yj = i - oz * level.nz, j - oy * level.ny
        if kind == "c":
            source_at = (pl.ds(1 + i, rows), pl.ds(1 + j, count))
            target_at = (pl.ds(1 + zi, rows), pl.ds(1 + yj, count))
        else:
            source_at = (pl.ds(level.halo + i, rows), pl.ds(level.col(j), count))
            target_at = (pl.ds(level.halo + zi, rows), pl.ds(level.col(yj), count))
        return pltpu.make_async_remote_copy(
            src_ref=ref.at[source_at],
            dst_ref=ref.at[target_at],
            send_sem=send_sem.at[groups.index((kind, number))],
            recv_sem=recv_sem.at[groups.index((kind, number))],
            device_id=peer(oz, oy),
            device_id_type=MESH,
        )

    def send(kind, number, end=None):
        for index, (k, l, m) in enumerate(table):
            if (k, l) == (kind, number) and (end is None or m[2] + m[4] == end):
                describe(index).start()

    def whole(group):
        size, place = group_lines(table, group), groups.index(group)
        every = sizer.at[pl.ds(0, size)]
        return pltpu.make_async_remote_copy(
            every, every, send_sem.at[place], recv_sem.at[place], device_id=peer(0, 1), device_id_type=MESH
        )

    def receive(kind, number):
        if (kind, number) in groups:
            whole((kind, number)).wait_recv()

    def sweep(level, ring, body, after=None):
        cols = sorted({level.col(y) for y in range(-ring, level.ny + ring)})
        first, count = level.halo - ring, level.nz + 2 * ring
        step = count if count * len(cols) <= STRAIGHT else max(k for k in range(1, ROWS + 1) if count % k == 0)

        def rows(start):
            for z in range(step):
                for y in cols:
                    body(start + z, y)
            if after is not None:
                after(start, step)

        if step == count:
            rows(first)
        else:
            lax.fori_loop(0, count // step, lambda i, carry: (rows(first + i * step), carry)[1], 0)

    def beside(level, ref, z, y, middle):
        up, down = ((y + 1) % level.cols, (y - 1) % level.cols) if level.full else (y + 1, y - 1)
        return ref[z - 1, y] + ref[z + 1, y] + ref[z, up] + ref[z, down] + rolls(middle)

    def smooth(number):
        level = levels[number]
        uu, ff, tt, p, q = u[number], f[number], t[number], d1[number], d2[number]
        ring = level.ring

        def first(z, y):
            v = uu[z, y]
            p[z, y] = (ff[z, y] - ((6.0 + tt[z, y]) * v - beside(level, uu, z, y, v))) * (1.0 / CENTRE)

        def second(z, y):
            v = p[z, y]
            q[z, y] = ((A2 + B2 * CENTRE) - B2 * (6.0 + tt[z, y])) * v + B2 * beside(level, p, z, y, v)

        def third(z, y):
            v, w = q[z, y], p[z, y]
            out = uu[z, y] + (1.0 - B3 * A2 / B2) * w
            out = out + ((1.0 + A3 + B3 / B2) - B3 * (6.0 + tt[z, y])) * v + B3 * beside(level, q, z, y, v)
            finish(z, y, out)

        def finish(z, y, out):
            row, col = z - level.halo, y - level.off
            if ring == 0 or (0 <= row < level.nz and 0 <= col < level.ny):
                outs[number][row, col] = out
            if number < n - 1:
                at = (col + 1) % level.total_y if level.full else col + 1
                c[number][row + 1, at] = out.astype(jnp.bfloat16)

        sweep(level, ring + 2, first)
        sweep(level, ring + 1, second)
        sweep(level, ring, third)

    def index_lines(number):
        level, coarse = levels[number], levels[number - 1]
        base_row = my_z * coarse.nz - 1
        base_col = my_y * coarse.ny - 1

        def row(i, carry):
            for j in range(level.ny):
                for k in range(2):
                    link = link_lines[number][(i, j, k) if level.ny == 2 else (i, k, j)]
                    at_row = modulo(link // coarse.total_y - base_row, coarse.nz * peers_z)
                    at_col = modulo(link - base_col, coarse.total_y)
                    at = jnp.minimum(at_row, coarse.nz + 1) * (coarse.ny + 2) + jnp.minimum(at_col, coarse.ny + 1)
                    lines[number][(i * level.ny + j) * 2 + k] = at
            return carry

        lax.fori_loop(0, level.nz, row, 0)

    def prolong(number):
        level = levels[number]

        def row(i, carry):
            for j in range(level.ny):
                at = (i * level.ny + j) * 2
                picked = [c_flat[number - 1][lines[number][at + k]] for k in range(2)]
                total = g[number][i, j] + lax.dot_general(
                    jnp.concatenate(picked, axis=1),
                    jnp.concatenate([b[number][i, j, 0], b[number][i, j, 1]], axis=1),
                    (((1,), (1,)), ((), ())),
                    preferred_element_type=jnp.float32,
                )
                u[number][level.halo + i, level.off + j] = total
            return carry

        ends = sorted({m[2] + m[4] for k, l, m in table if (k, l) == ("u", number)} | {level.nz})
        start = 0
        for end in ends:
            step = max(k for k in range(1, PROLONG_ROWS + 1) if (end - start) % k == 0)

            def some(i, carry, start=start, step=step):
                for k in range(step):
                    row(start + i * step + k, carry)
                return carry

            lax.fori_loop(0, (end - start) // step, some, 0)
            send("u", number, end)
            start = end

    for key in (("f", 0), ("t", 0), ("g", 0)):
        loads[key].wait()
    pl.semaphore_wait(barrier, len(partners))
    def send_inputs(number):
        for kind in ("t", "f"):
            loads[(kind, number)].wait()
            send(kind, number)

    for kind in ("u", "f", "t"):
        send(kind, 0)
    send_inputs(1)
    for number in range(1, n):
        loads[("l", number)].wait()
        index_lines(number)
    for number in range(n):
        if number:
            loads[("g", number)].wait()
            loads[("b", number)].wait()
            prolong(number)
            if number == 1:
                send_inputs(3)
        for kind in ("f", "t", "u"):
            receive(kind, number)
        smooth(number)
        send("c", number)
        if number == 0:
            send_inputs(2)
        receive("c", number)
    for group in groups:
        whole(group).wait_send()


def copy_out(*refs):
    results, outs, sem = refs[: len(refs) // 2], refs[len(refs) // 2 : -1], refs[-1]
    copies = [pltpu.make_async_copy(r, o, sem.at[k]) for k, (r, o) in enumerate(zip(results, outs))]
    for copy in copies:
        copy.start()
    for copy in copies:
        copy.wait()


def shards(peers, *arrays):
    fine_to_coarse = lambda group: group[::-1]
    source, guess, shift = (fine_to_coarse(arrays[k : k + 4]) for k in (0, 4, 8))
    blocks, links = (fine_to_coarse(arrays[k : k + 3]) for k in (12, 15))
    n = len(source)
    sides, line = source[0].shape[2:]
    levels, table = plan([x.shape[:2] for x in source], *peers)
    shift = [x.reshape(x.shape[0], x.shape[1], 1, line) for x in shift]
    links = [x if x.shape[1] == x.shape[2] else x.transpose(0, 2, 1) for x in links]
    f32, bf16 = jnp.float32, jnp.bfloat16
    extended = [pltpu.VMEM((l.rows, l.cols, sides, line), f32) for l in levels]
    scratch = extended + extended + [pltpu.VMEM((l.rows, l.cols, 1, line), f32) for l in levels] + extended + extended
    scratch += [pltpu.VMEM(x.shape, f32) for x in guess[1:]]
    scratch += [pltpu.VMEM(x.shape, bf16) for x in blocks]
    scratch += [pltpu.VMEM((l.nz + 2, l.ny + 2, sides, line), bf16) for l in levels[:-1]]
    scratch += [pltpu.SMEM((2 * l.nz * l.ny,), jnp.int32) for l in levels[1:]]
    scratch += [pltpu.SMEM(x.shape, jnp.int32) for x in links]
    scratch += [
        pltpu.VMEM((max(group_lines(table, group) for group in groups_of(table)), 1, line), f32),
        pltpu.SemaphoreType.DMA((3 * n + 3 * (n - 1),)),
        pltpu.SemaphoreType.DMA((len(groups_of(table)),)),
        pltpu.SemaphoreType.DMA((len(groups_of(table)),)),
    ]
    hbm, vmem = pl.BlockSpec(memory_space=pltpu.HBM), pl.BlockSpec(memory_space=pltpu.VMEM)
    operands = [pltpu.with_memory_space_constraint(x, pltpu.HBM) for x in (*source, *guess, *shift, *blocks, *links)]
    shapes = [jax.ShapeDtypeStruct(x.shape, f32) for x in source]
    results = pl.pallas_call(
        functools.partial(kernel, levels, table, peers),
        out_shape=shapes,
        in_specs=[hbm] * len(operands),
        out_specs=[vmem] * n,
        scratch_shapes=scratch,
        compiler_params=pltpu.CompilerParams(
            collective_id=0, has_side_effects=True, vmem_limit_bytes=32 * 1024 * 1024
        ),
    )(*operands)
    results = pl.pallas_call(
        copy_out,
        out_shape=shapes,
        in_specs=[pl.BlockSpec(memory_space=pl.ANY)] * n,
        out_specs=[hbm] * n,
        scratch_shapes=[pltpu.SemaphoreType.DMA((n,))],
        compiler_params=pltpu.CompilerParams(vmem_limit_bytes=2 * 1024 * 1024),
    )(*results)
    return tuple(results[::-1])


def solution(mesh):
    wide = P("gz", "gy", None, None)
    flat = P("gz", "gy", None)
    in_specs = (wide,) * 8 + (flat,) * 4 + (P("gz", "gy", None, None, None),) * 3 + (flat,) * 3
    peers = (mesh.shape["gz"], mesh.shape["gy"])
    return jax.shard_map(
        functools.partial(shards, peers), mesh=mesh, in_specs=in_specs, out_specs=(wide,) * 4, check_vma=False
    )
```

```python
import functools

import jax
import jax.numpy as jnp
from jax import lax
from jax.experimental import pallas as pl
from jax.experimental.pallas import tpu as pltpu
from jax.sharding import PartitionSpec as P

MESH = pl.DeviceIdType.MESH

upper_edge = 14.0
lower_edge = upper_edge / 8.0
CENTRE = (upper_edge + lower_edge) / 2.0
HALF = (upper_edge - lower_edge) / 2.0
RATIO = CENTRE / HALF
FACTOR_0 = 1.0 / RATIO
FACTOR_1 = 1.0 / (2.0 * RATIO - FACTOR_0)
FACTOR_2 = 1.0 / (2.0 * RATIO - FACTOR_1)
A2, B2 = FACTOR_1 * FACTOR_0, 2.0 * FACTOR_1 / HALF
A3, B3 = FACTOR_2 * FACTOR_1, 2.0 * FACTOR_2 / HALF

RADIUS = 3
RINGS = (0, 1, 1, 0)
NARROW = (False, True, True, True)
NARROW_SOURCE = (True, True, True, True)
STRAIGHT = 64
PROLONG_ROWS = 2
PIECE = 2
ROWS = 5


class Level:
    def __init__(self, nz, ny, peers_z, peers_y, ring):
        self.nz, self.ny, self.ring = nz, ny, ring
        self.peers_y = peers_y
        self.halo = RADIUS + ring
        self.total_y = ny * peers_y
        self.full = ny + 2 * self.halo >= self.total_y
        self.rows = nz + 2 * self.halo
        self.cols = self.total_y if self.full else ny + 2 * self.halo
        self.off = 0 if self.full else self.halo

    def col(self, y):
        return y % self.total_y if self.full else y + self.off

    def gap(self, z, y, ring):
        def along(p, n):
            return max(0, -p - ring, p - (n - 1) - ring)

        turns = (-1, 0, 1) if self.full else (0,)
        return along(z, self.nz), min(along(y + t * self.total_y, self.ny) for t in turns)

    def needs(self, z, y, radius, near):
        if sum(self.gap(z, y, self.ring)) > radius:
            return False
        return near is None or near == (max(self.gap(z, y, 0)) == 1)

    def messages(self, radius, near=None):
        found = []
        reach = -(-self.halo // self.nz)
        offsets_y = range(-(self.peers_y // 2 - 1), self.peers_y // 2 + 1) if self.full else range(-1, 2)
        for oz in range(-reach, reach + 1):
            for oy in offsets_y:
                if (oz, oy) == (0, 0):
                    continue
                spans = []
                for i in range(self.nz):
                    js = [j for j in range(self.ny) if self.needs(i - oz * self.nz, j - oy * self.ny, radius, near)]
                    if not js:
                        continue
                    assert js == list(range(js[0], js[-1] + 1))
                    span = (js[0], len(js))
                    if spans and spans[-1][1] == span and spans[-1][0] + spans[-1][2] == i:
                        spans[-1][2] += 1
                    else:
                        spans.append([i, span, 1])
                for i, (j, count), rows in spans:
                    for part in range(i, i + rows, PIECE):
                        found.append((oz, oy, part, j, min(PIECE, i + rows - part), count))
        return sorted(found, key=lambda m: -abs(m[1]))

    def far_cells(self, radius):
        return sorted(
            {
                (self.halo + i + a - oz * self.nz, self.col(j + k - oy * self.ny))
                for oz, oy, i, j, rows, count in self.messages(radius, False)
                for a in range(rows)
                for k in range(count)
            }
        )


def ring_messages(nz, ny):
    found = []
    for oz in (-1, 0, 1):
        for oy in (-1, 0, 1):
            if (oz, oy) == (0, 0):
                continue
            i, rows = (0, nz) if oz == 0 else ((nz - 1, 1) if oz == 1 else (0, 1))
            j, count = (0, ny) if oy == 0 else ((ny - 1, 1) if oy == 1 else (0, 1))
            found.append((oz, oy, i, j, rows, count))
    return found


def plan(shapes, peers_z, peers_y):
    levels = [Level(nz, ny, peers_z, peers_y, ring) for (nz, ny), ring in zip(shapes, RINGS)]
    table = []
    for number, level in enumerate(levels):
        for wide, narrow, radius, split in (("u", "v", RADIUS, NARROW[number]), ("f", "w", RADIUS - 1, NARROW_SOURCE[number])):
            table += [(wide, number, m) for m in level.messages(radius, True if split else None)]
            if split:
                table += [(narrow, number, m) for m in level.messages(radius, False)]
        table += [("t", number, m) for m in level.messages(RADIUS - 1)]
        if number < len(levels) - 1 and level.ring == 0:
            table += [("c", number, m) for m in ring_messages(level.nz, level.ny)]
    return levels, table


def groups_of(table):
    return sorted({(kind, number) for kind, number, _ in table})


def group_lines(table, group):
    lines = {"u": 16, "v": 8, "f": 16, "w": 8, "t": 1, "c": 8}[group[0]]
    return sum(lines * m[4] * m[5] for kind, number, m in table if (kind, number) == group)


def modulo(value, size):
    return (value + size) & (size - 1) if size & (size - 1) == 0 else lax.rem(value + size, size)


def rolls(v):
    return pltpu.roll(v, 1, 1) + pltpu.roll(v, v.shape[1] - 1, 1)


def kernel(levels, table, peers, *refs):
    n = len(levels)
    source, guess, shift = refs[0:n], refs[n : 2 * n], refs[2 * n : 3 * n]
    refs = refs[3 * n :]
    blocks, links = (None,) + refs[: n - 1], (None,) + refs[n - 1 : 2 * n - 2]
    refs = refs[2 * n - 2 :]
    outs, refs = refs[:n], refs[n:]
    u, f, t, d1, d2 = (refs[k * n : (k + 1) * n] for k in range(5))
    refs = refs[5 * n :]
    g, b, c = (None,) + refs[: n - 1], (None,) + refs[n - 1 : 2 * n - 2], refs[2 * n - 2 : 3 * n - 3]
    lines, link_lines = (None,) + refs[3 * n - 3 : 4 * n - 4], (None,) + refs[4 * n - 4 : 5 * n - 5]
    v, w = refs[5 * n - 5 : 6 * n - 5], refs[6 * n - 5 : 7 * n - 5]
    sizer, local_sem, send_sem, recv_sem = refs[7 * n - 5 :]
    c_flat = [x.reshape((-1,) + x.shape[2:]) for x in c]

    peers_z, peers_y = peers
    my_z, my_y = lax.axis_index("gz"), lax.axis_index("gy")

    def peer(oz, oy):
        return (lax.rem(my_z + (oz + peers_z), peers_z), lax.rem(my_y + (oy + peers_y), peers_y))

    barrier = pltpu.get_barrier_semaphore()
    partners = sorted({m[:2] for _, _, m in table})
    for oz, oy in partners:
        pl.semaphore_signal(barrier, inc=1, device_id=peer(oz, oy), device_id_type=MESH)

    loads = {}

    def load(key, src, dst):
        loads[key] = pltpu.make_async_copy(src, dst, local_sem.at[len(loads)])
        loads[key].start()

    for number, level in enumerate(levels):
        own = (pl.ds(level.halo, level.nz), pl.ds(level.off, level.ny))
        load(("f", number), source[number], f[number].at[own])
        load(("t", number), shift[number], t[number].at[own])
        if number == 0:
            load(("g", 0), guess[0], u[0].at[own])
    for number in range(1, n):
        load(("l", number), links[number], link_lines[number])
        load(("g", number), guess[number], g[number])
        load(("b", number), blocks[number], b[number])

    buffers = {"u": u, "v": v, "f": f, "w": w, "t": t, "c": c}
    groups = groups_of(table)

    def describe(index):
        kind, number, (oz, oy, i, j, rows, count) = table[index]
        level, ref = levels[number], buffers[kind][number]
        zi, yj = i - oz * level.nz, j - oy * level.ny
        if kind == "c":
            source_at = (pl.ds(1 + i, rows), pl.ds(1 + j, count))
            target_at = (pl.ds(1 + zi, rows), pl.ds(1 + yj, count))
        else:
            source_at = (pl.ds(level.halo + i, rows), pl.ds(level.col(j), count))
            target_at = (pl.ds(level.halo + zi, rows), pl.ds(level.col(yj), count))
        return pltpu.make_async_remote_copy(
            src_ref=ref.at[source_at],
            dst_ref=ref.at[target_at],
            send_sem=send_sem.at[groups.index((kind, number))],
            recv_sem=recv_sem.at[groups.index((kind, number))],
            device_id=peer(oz, oy),
            device_id_type=MESH,
        )

    def send(kind, number, end=None):
        for index, (k, l, m) in enumerate(table):
            if (k, l) == (kind, number) and (end is None or m[2] + m[4] == end):
                describe(index).start()

    def whole(group):
        size, place = group_lines(table, group), groups.index(group)
        every = sizer.at[pl.ds(0, size)]
        return pltpu.make_async_remote_copy(
            every, every, send_sem.at[place], recv_sem.at[place], device_id=peer(0, 1), device_id_type=MESH
        )

    def receive(kind, number):
        if (kind, number) in groups:
            whole((kind, number)).wait_recv()

    def sweep(level, ring, body, after=None):
        cols = sorted({level.col(y) for y in range(-ring, level.ny + ring)})
        first, count = level.halo - ring, level.nz + 2 * ring
        step = count if count * len(cols) <= STRAIGHT else max(k for k in range(1, ROWS + 1) if count % k == 0)

        def rows(start):
            for z in range(step):
                for y in cols:
                    body(start + z, y)
            if after is not None:
                after(start, step)

        if step == count:
            rows(first)
        else:
            lax.fori_loop(0, count // step, lambda i, carry: (rows(first + i * step), carry)[1], 0)

    def beside(level, ref, z, y, middle):
        up, down = ((y + 1) % level.cols, (y - 1) % level.cols) if level.full else (y + 1, y - 1)
        return ref[z - 1, y] + ref[z + 1, y] + ref[z, up] + ref[z, down] + rolls(middle)

    def smooth(number):
        level = levels[number]
        uu, ff, tt, p, q = u[number], f[number], t[number], d1[number], d2[number]
        ring = level.ring

        def first(z, y):
            v = uu[z, y]
            p[z, y] = (ff[z, y] - ((6.0 + tt[z, y]) * v - beside(level, uu, z, y, v))) * (1.0 / CENTRE)

        def second(z, y):
            v = p[z, y]
            q[z, y] = ((A2 + B2 * CENTRE) - B2 * (6.0 + tt[z, y])) * v + B2 * beside(level, p, z, y, v)

        def third(z, y):
            v, w = q[z, y], p[z, y]
            out = uu[z, y] + (1.0 - B3 * A2 / B2) * w
            out = out + ((1.0 + A3 + B3 / B2) - B3 * (6.0 + tt[z, y])) * v + B3 * beside(level, q, z, y, v)
            finish(z, y, out)

        def finish(z, y, out):
            row, col = z - level.halo, y - level.off
            if ring == 0 or (0 <= row < level.nz and 0 <= col < level.ny):
                outs[number][row, col] = out
            if number < n - 1:
                at = (col + 1) % level.total_y if level.full else col + 1
                c[number][row + 1, at] = out.astype(jnp.bfloat16)

        sweep(level, ring + 2, first)
        sweep(level, ring + 1, second)
        sweep(level, ring, third)

    def index_lines(number):
        level, coarse = levels[number], levels[number - 1]
        base_row = my_z * coarse.nz - 1
        base_col = my_y * coarse.ny - 1

        def row(i, carry):
            for j in range(level.ny):
                for k in range(2):
                    link = link_lines[number][(i, j, k) if level.ny == 2 else (i, k, j)]
                    at_row = modulo(link // coarse.total_y - base_row, coarse.nz * peers_z)
                    at_col = modulo(link - base_col, coarse.total_y)
                    at = jnp.minimum(at_row, coarse.nz + 1) * (coarse.ny + 2) + jnp.minimum(at_col, coarse.ny + 1)
                    lines[number][(i * level.ny + j) * 2 + k] = at
            return carry

        lax.fori_loop(0, level.nz, row, 0)

    def prolong(number):
        level = levels[number]

        def row(i, carry):
            for j in range(level.ny):
                at = (i * level.ny + j) * 2
                picked = [c_flat[number - 1][lines[number][at + k]] for k in range(2)]
                total = g[number][i, j] + lax.dot_general(
                    jnp.concatenate(picked, axis=1),
                    jnp.concatenate([b[number][i, j, 0], b[number][i, j, 1]], axis=0),
                    (((1,), (0,)), ((), ())),
                    preferred_element_type=jnp.float32,
                )
                u[number][level.halo + i, level.off + j] = total
                if NARROW[number]:
                    v[number][level.halo + i, level.off + j] = total.astype(jnp.bfloat16)
            return carry

        ends = sorted({m[2] + m[4] for k, l, m in table if l == number and k in ("u", "v")} | {level.nz})
        start = 0
        for end in ends:
            step = max(k for k in range(1, PROLONG_ROWS + 1) if (end - start) % k == 0)

            def some(i, carry, start=start, step=step):
                for k in range(step):
                    row(start + i * step + k, carry)
                return carry

            lax.fori_loop(0, (end - start) // step, some, 0)
            for kind in ("v", "u"):
                send(kind, number, end)
            start = end

    for key in (("f", 0), ("t", 0), ("g", 0)):
        loads[key].wait()
    def narrow_own(level, wide, narrow):
        def row(i, carry):
            for j in range(level.ny):
                narrow[level.halo + i, level.off + j] = wide[level.halo + i, level.off + j].astype(jnp.bfloat16)
            return carry

        lax.fori_loop(0, level.nz, row, 0)

    def widen_far(level, radius, narrow, wide):
        for z, y in level.far_cells(radius):
            wide[z, y] = narrow[z, y].astype(jnp.float32)

    def send_inputs(number):
        for kind in ("t", "f"):
            loads[(kind, number)].wait()
        if NARROW_SOURCE[number]:
            narrow_own(levels[number], f[number], w[number])
        for kind in ("t", "w", "f"):
            send(kind, number)

    def turn(number):
        loads[("b", number)].wait()
        level = levels[number]

        def row(i, carry):
            for j in range(level.ny):
                for k in range(2):
                    b[number][i, j, k] = b[number][i, j, k].T
            return carry

        lax.fori_loop(0, level.nz, row, 0)

    if NARROW_SOURCE[0]:
        narrow_own(levels[0], f[0], w[0])
    if NARROW[0]:
        narrow_own(levels[0], u[0], v[0])
    pl.semaphore_wait(barrier, len(partners))
    for kind in ("v", "w", "u", "f", "t"):
        send(kind, 0)
    send_inputs(1)
    for number in range(1, n):
        loads[("l", number)].wait()
        index_lines(number)
    for number in range(n):
        if number:
            loads[("g", number)].wait()
            prolong(number)
            if number == 1:
                send_inputs(3)
                turn(3)
        else:
            turn(1)
        for kind in ("f", "w", "t"):
            receive(kind, number)
        if NARROW_SOURCE[number]:
            widen_far(levels[number], RADIUS - 1, w[number], f[number])
        for kind in ("u", "v"):
            receive(kind, number)
        if NARROW[number]:
            widen_far(levels[number], RADIUS, v[number], u[number])
        smooth(number)
        send("c", number)
        if number == 0:
            send_inputs(2)
            turn(2)
        receive("c", number)
    for group in groups:
        whole(group).wait_send()


def copy_out(*refs):
    results, outs, sem = refs[: len(refs) // 2], refs[len(refs) // 2 : -1], refs[-1]
    copies = [pltpu.make_async_copy(r, o, sem.at[k]) for k, (r, o) in enumerate(zip(results, outs))]
    for copy in copies:
        copy.start()
    for copy in copies:
        copy.wait()


def shards(peers, *arrays):
    fine_to_coarse = lambda group: group[::-1]
    source, guess, shift = (fine_to_coarse(arrays[k : k + 4]) for k in (0, 4, 8))
    blocks, links = (fine_to_coarse(arrays[k : k + 3]) for k in (12, 15))
    n = len(source)
    sides, line = source[0].shape[2:]
    levels, table = plan([x.shape[:2] for x in source], *peers)
    shift = [x.reshape(x.shape[0], x.shape[1], 1, line) for x in shift]
    links = [x if x.shape[1] == x.shape[2] else x.transpose(0, 2, 1) for x in links]
    f32, bf16 = jnp.float32, jnp.bfloat16
    extended = [pltpu.VMEM((l.rows, l.cols, sides, line), f32) for l in levels]
    scratch = extended + extended + [pltpu.VMEM((l.rows, l.cols, 1, line), f32) for l in levels] + extended + extended
    scratch += [pltpu.VMEM(x.shape, f32) for x in guess[1:]]
    scratch += [pltpu.VMEM(x.shape, bf16) for x in blocks]
    scratch += [pltpu.VMEM((l.nz + 2, l.ny + 2, sides, line), bf16) for l in levels[:-1]]
    scratch += [pltpu.SMEM((2 * l.nz * l.ny,), jnp.int32) for l in levels[1:]]
    scratch += [pltpu.SMEM(x.shape, jnp.int32) for x in links]
    scratch += [pltpu.VMEM((l.rows, l.cols, sides, line), bf16) for l in levels] * 2
    scratch += [
        pltpu.VMEM((max(group_lines(table, group) for group in groups_of(table)), 1, line), f32),
        pltpu.SemaphoreType.DMA((3 * n + 3 * (n - 1),)),
        pltpu.SemaphoreType.DMA((len(groups_of(table)),)),
        pltpu.SemaphoreType.DMA((len(groups_of(table)),)),
    ]
    hbm, vmem = pl.BlockSpec(memory_space=pltpu.HBM), pl.BlockSpec(memory_space=pltpu.VMEM)
    operands = [pltpu.with_memory_space_constraint(x, pltpu.HBM) for x in (*source, *guess, *shift, *blocks, *links)]
    shapes = [jax.ShapeDtypeStruct(x.shape, f32) for x in source]
    results = pl.pallas_call(
        functools.partial(kernel, levels, table, peers),
        out_shape=shapes,
        in_specs=[hbm] * len(operands),
        out_specs=[vmem] * n,
        scratch_shapes=scratch,
        compiler_params=pltpu.CompilerParams(
            collective_id=0, has_side_effects=True, vmem_limit_bytes=32 * 1024 * 1024
        ),
    )(*operands)
    results = pl.pallas_call(
        copy_out,
        out_shape=shapes,
        in_specs=[pl.BlockSpec(memory_space=pl.ANY)] * n,
        out_specs=[hbm] * n,
        scratch_shapes=[pltpu.SemaphoreType.DMA((n,))],
        compiler_params=pltpu.CompilerParams(vmem_limit_bytes=2 * 1024 * 1024),
    )(*results)
    return tuple(results[::-1])


def solution(mesh):
    wide = P("gz", "gy", None, None)
    flat = P("gz", "gy", None)
    in_specs = (wide,) * 8 + (flat,) * 4 + (P("gz", "gy", None, None, None),) * 3 + (flat,) * 3
    peers = (mesh.shape["gz"], mesh.shape["gy"])
    return jax.shard_map(
        functools.partial(shards, peers), mesh=mesh, in_specs=in_specs, out_specs=(wide,) * 4, check_vma=False
    )
```

```python
import functools

import jax
import jax.numpy as jnp
from jax import lax
from jax.experimental import pallas as pl
from jax.experimental.pallas import tpu as pltpu
from jax.sharding import PartitionSpec as P

MESH = pl.DeviceIdType.MESH

upper_edge = 14.0
lower_edge = upper_edge / 8.0
CENTRE = (upper_edge + lower_edge) / 2.0
HALF = (upper_edge - lower_edge) / 2.0
RATIO = CENTRE / HALF
FACTOR_0 = 1.0 / RATIO
FACTOR_1 = 1.0 / (2.0 * RATIO - FACTOR_0)
FACTOR_2 = 1.0 / (2.0 * RATIO - FACTOR_1)
A2, B2 = FACTOR_1 * FACTOR_0, 2.0 * FACTOR_1 / HALF
A3, B3 = FACTOR_2 * FACTOR_1, 2.0 * FACTOR_2 / HALF

RADIUS = 3
RINGS = (0, 1, 1, 0)
NARROW = (False, True, True, True)
NARROW_SOURCE = (True, True, True, True)
STRAIGHT = 64
PROLONG_ROWS = 2
PIECE = 2
ROWS = 5


class Level:
    def __init__(self, nz, ny, peers_z, peers_y, ring):
        self.nz, self.ny, self.ring = nz, ny, ring
        self.peers_y = peers_y
        self.halo = RADIUS + ring
        self.total_y = ny * peers_y
        self.full = ny + 2 * self.halo >= self.total_y
        self.rows = nz + 2 * self.halo
        self.cols = self.total_y if self.full else ny + 2 * self.halo
        self.off = 0 if self.full else self.halo

    def col(self, y):
        return y % self.total_y if self.full else y + self.off

    def gap(self, z, y, ring):
        def along(p, n):
            return max(0, -p - ring, p - (n - 1) - ring)

        turns = (-1, 0, 1) if self.full else (0,)
        return along(z, self.nz), min(along(y + t * self.total_y, self.ny) for t in turns)

    def needs(self, z, y, radius, near):
        if sum(self.gap(z, y, self.ring)) > radius:
            return False
        return near is None or near == (max(self.gap(z, y, 0)) == 1)

    def messages(self, radius, near=None):
        found = []
        reach = -(-self.halo // self.nz)
        offsets_y = range(-(self.peers_y // 2 - 1), self.peers_y // 2 + 1) if self.full else range(-1, 2)
        for oz in range(-reach, reach + 1):
            for oy in offsets_y:
                if (oz, oy) == (0, 0):
                    continue
                spans = []
                for i in range(self.nz):
                    js = [j for j in range(self.ny) if self.needs(i - oz * self.nz, j - oy * self.ny, radius, near)]
                    if not js:
                        continue
                    assert js == list(range(js[0], js[-1] + 1))
                    span = (js[0], len(js))
                    if spans and spans[-1][1] == span and spans[-1][0] + spans[-1][2] == i:
                        spans[-1][2] += 1
                    else:
                        spans.append([i, span, 1])
                for i, (j, count), rows in spans:
                    for part in range(i, i + rows, PIECE):
                        found.append((oz, oy, part, j, min(PIECE, i + rows - part), count))
        return sorted(found, key=lambda m: -abs(m[1]))

    def far_cells(self, radius):
        return sorted(
            {
                (self.halo + i + a - oz * self.nz, self.col(j + k - oy * self.ny))
                for oz, oy, i, j, rows, count in self.messages(radius, False)
                for a in range(rows)
                for k in range(count)
            }
        )


def ring_messages(nz, ny):
    found = []
    for oz in (-1, 0, 1):
        for oy in (-1, 0, 1):
            if (oz, oy) == (0, 0):
                continue
            i, rows = (0, nz) if oz == 0 else ((nz - 1, 1) if oz == 1 else (0, 1))
            j, count = (0, ny) if oy == 0 else ((ny - 1, 1) if oy == 1 else (0, 1))
            found.append((oz, oy, i, j, rows, count))
    return found


def plan(shapes, peers_z, peers_y):
    levels = [Level(nz, ny, peers_z, peers_y, ring) for (nz, ny), ring in zip(shapes, RINGS)]
    table = []
    for number, level in enumerate(levels):
        for wide, narrow, radius, split in (("u", "v", RADIUS, NARROW[number]), ("f", "w", RADIUS - 1, NARROW_SOURCE[number])):
            table += [(wide, number, m) for m in level.messages(radius, True if split else None)]
            if split:
                table += [(narrow, number, m) for m in level.messages(radius, False)]
        table += [("t", number, m) for m in level.messages(RADIUS - 1)]
        if number < len(levels) - 1 and level.ring == 0:
            table += [("c", number, m) for m in ring_messages(level.nz, level.ny)]
    return levels, table


def groups_of(table):
    return sorted({(kind, number) for kind, number, _ in table})


def group_lines(table, group):
    lines = {"u": 16, "v": 8, "f": 16, "w": 8, "t": 1, "c": 8}[group[0]]
    return sum(lines * m[4] * m[5] for kind, number, m in table if (kind, number) == group)


def by_way(kind, number, message):
    oz, oy, _, _, rows, count = message
    return (-(abs(oy) + (abs(oz) + 1) // 2), rows * count)


ORDER = by_way


def modulo(value, size):
    return (value + size) & (size - 1) if size & (size - 1) == 0 else lax.rem(value + size, size)


def rolls(v):
    return pltpu.roll(v, 1, 1) + pltpu.roll(v, v.shape[1] - 1, 1)


def kernel(levels, table, peers, *refs):
    n = len(levels)
    source, guess, shift = refs[0:n], refs[n : 2 * n], refs[2 * n : 3 * n]
    refs = refs[3 * n :]
    blocks, links = (None,) + refs[: n - 1], (None,) + refs[n - 1 : 2 * n - 2]
    refs = refs[2 * n - 2 :]
    outs, refs = refs[:n], refs[n:]
    u, f, t, d1, d2 = (refs[k * n : (k + 1) * n] for k in range(5))
    refs = refs[5 * n :]
    g, b, c = (None,) + refs[: n - 1], (None,) + refs[n - 1 : 2 * n - 2], refs[2 * n - 2 : 3 * n - 3]
    lines, link_lines = (None,) + refs[3 * n - 3 : 4 * n - 4], (None,) + refs[4 * n - 4 : 5 * n - 5]
    v, w = refs[5 * n - 5 : 6 * n - 5], refs[6 * n - 5 : 7 * n - 5]
    sizer, local_sem, send_sem, recv_sem = refs[7 * n - 5 :]
    c_flat = [x.reshape((-1,) + x.shape[2:]) for x in c]

    peers_z, peers_y = peers
    my_z, my_y = lax.axis_index("gz"), lax.axis_index("gy")

    def peer(oz, oy):
        return (lax.rem(my_z + (oz + peers_z), peers_z), lax.rem(my_y + (oy + peers_y), peers_y))

    barrier = pltpu.get_barrier_semaphore()
    partners = sorted({m[:2] for _, _, m in table})
    for oz, oy in partners:
        pl.semaphore_signal(barrier, inc=1, device_id=peer(oz, oy), device_id_type=MESH)

    loads = {}

    def load(key, src, dst):
        loads[key] = pltpu.make_async_copy(src, dst, local_sem.at[len(loads)])
        loads[key].start()

    for number, level in enumerate(levels):
        own = (pl.ds(level.halo, level.nz), pl.ds(level.off, level.ny))
        load(("f", number), source[number], f[number].at[own])
        load(("t", number), shift[number], t[number].at[own])
        if number == 0:
            load(("g", 0), guess[0], u[0].at[own])
    for number in range(1, n):
        load(("l", number), links[number], link_lines[number])
        load(("g", number), guess[number], g[number])
        load(("b", number), blocks[number], b[number])

    buffers = {"u": u, "v": v, "f": f, "w": w, "t": t, "c": c}
    groups = groups_of(table)

    def describe(index):
        kind, number, (oz, oy, i, j, rows, count) = table[index]
        level, ref = levels[number], buffers[kind][number]
        zi, yj = i - oz * level.nz, j - oy * level.ny
        if kind == "c":
            source_at = (pl.ds(1 + i, rows), pl.ds(1 + j, count))
            target_at = (pl.ds(1 + zi, rows), pl.ds(1 + yj, count))
        else:
            source_at = (pl.ds(level.halo + i, rows), pl.ds(level.col(j), count))
            target_at = (pl.ds(level.halo + zi, rows), pl.ds(level.col(yj), count))
        return pltpu.make_async_remote_copy(
            src_ref=ref.at[source_at],
            dst_ref=ref.at[target_at],
            send_sem=send_sem.at[groups.index((kind, number))],
            recv_sem=recv_sem.at[groups.index((kind, number))],
            device_id=peer(oz, oy),
            device_id_type=MESH,
        )

    def send(kinds, number, end=None):
        chosen = [
            index
            for index, (k, l, m) in enumerate(table)
            if k in kinds and l == number and (end is None or m[2] + m[4] == end)
        ]
        for index in sorted(chosen, key=lambda index: ORDER(*table[index])):
            describe(index).start()

    def whole(group):
        size, place = group_lines(table, group), groups.index(group)
        every = sizer.at[pl.ds(0, size)]
        return pltpu.make_async_remote_copy(
            every, every, send_sem.at[place], recv_sem.at[place], device_id=peer(0, 1), device_id_type=MESH
        )

    def receive(kind, number):
        if (kind, number) in groups:
            whole((kind, number)).wait_recv()

    def sweep(level, ring, body, after=None):
        cols = sorted({level.col(y) for y in range(-ring, level.ny + ring)})
        first, count = level.halo - ring, level.nz + 2 * ring
        step = count if count * len(cols) <= STRAIGHT else max(k for k in range(1, ROWS + 1) if count % k == 0)

        def rows(start):
            for z in range(step):
                for y in cols:
                    body(start + z, y)
            if after is not None:
                after(start, step)

        if step == count:
            rows(first)
        else:
            lax.fori_loop(0, count // step, lambda i, carry: (rows(first + i * step), carry)[1], 0)

    def beside(level, ref, z, y, middle):
        up, down = ((y + 1) % level.cols, (y - 1) % level.cols) if level.full else (y + 1, y - 1)
        return ref[z - 1, y] + ref[z + 1, y] + ref[z, up] + ref[z, down] + rolls(middle)

    def smooth(number):
        level = levels[number]
        uu, ff, tt, p, q = u[number], f[number], t[number], d1[number], d2[number]
        ring = level.ring

        def first(z, y):
            v = uu[z, y]
            p[z, y] = (ff[z, y] - ((6.0 + tt[z, y]) * v - beside(level, uu, z, y, v))) * (1.0 / CENTRE)

        def second(z, y):
            v = p[z, y]
            q[z, y] = ((A2 + B2 * CENTRE) - B2 * (6.0 + tt[z, y])) * v + B2 * beside(level, p, z, y, v)

        def third(z, y):
            v, w = q[z, y], p[z, y]
            out = uu[z, y] + (1.0 - B3 * A2 / B2) * w
            out = out + ((1.0 + A3 + B3 / B2) - B3 * (6.0 + tt[z, y])) * v + B3 * beside(level, q, z, y, v)
            finish(z, y, out)

        def finish(z, y, out):
            row, col = z - level.halo, y - level.off
            if ring == 0 or (0 <= row < level.nz and 0 <= col < level.ny):
                outs[number][row, col] = out
            if number < n - 1:
                at = (col + 1) % level.total_y if level.full else col + 1
                c[number][row + 1, at] = out.astype(jnp.bfloat16)

        sweep(level, ring + 2, first)
        sweep(level, ring + 1, second)
        sweep(level, ring, third)

    def index_lines(number):
        level, coarse = levels[number], levels[number - 1]
        base_row = my_z * coarse.nz - 1
        base_col = my_y * coarse.ny - 1

        def row(i, carry):
            for j in range(level.ny):
                for k in range(2):
                    link = link_lines[number][(i, j, k) if level.ny == 2 else (i, k, j)]
                    at_row = modulo(link // coarse.total_y - base_row, coarse.nz * peers_z)
                    at_col = modulo(link - base_col, coarse.total_y)
                    at = jnp.minimum(at_row, coarse.nz + 1) * (coarse.ny + 2) + jnp.minimum(at_col, coarse.ny + 1)
                    lines[number][(i * level.ny + j) * 2 + k] = at
            return carry

        lax.fori_loop(0, level.nz, row, 0)

    def prolong(number):
        level = levels[number]

        def row(i, carry):
            for j in range(level.ny):
                at = (i * level.ny + j) * 2
                picked = [c_flat[number - 1][lines[number][at + k]] for k in range(2)]
                total = g[number][i, j] + lax.dot_general(
                    jnp.concatenate(picked, axis=1),
                    jnp.concatenate([b[number][i, j, 0], b[number][i, j, 1]], axis=0),
                    (((1,), (0,)), ((), ())),
                    preferred_element_type=jnp.float32,
                )
                u[number][level.halo + i, level.off + j] = total
                if NARROW[number]:
                    v[number][level.halo + i, level.off + j] = total.astype(jnp.bfloat16)
            return carry

        ends = sorted({m[2] + m[4] for k, l, m in table if l == number and k in ("u", "v")} | {level.nz})
        start = 0
        for end in ends:
            step = max(k for k in range(1, PROLONG_ROWS + 1) if (end - start) % k == 0)

            def some(i, carry, start=start, step=step):
                for k in range(step):
                    row(start + i * step + k, carry)
                return carry

            lax.fori_loop(0, (end - start) // step, some, 0)
            send("uv", number, end)
            start = end

    for key in (("f", 0), ("t", 0), ("g", 0)):
        loads[key].wait()
    def narrow_own(level, wide, narrow):
        def row(i, carry):
            for j in range(level.ny):
                narrow[level.halo + i, level.off + j] = wide[level.halo + i, level.off + j].astype(jnp.bfloat16)
            return carry

        lax.fori_loop(0, level.nz, row, 0)

    def widen_far(level, radius, narrow, wide):
        for z, y in level.far_cells(radius):
            wide[z, y] = narrow[z, y].astype(jnp.float32)

    def send_inputs(number):
        for kind in ("t", "f"):
            loads[(kind, number)].wait()
        if NARROW_SOURCE[number]:
            narrow_own(levels[number], f[number], w[number])
        send("twf", number)

    def turn(number):
        loads[("b", number)].wait()
        level = levels[number]

        def row(i, carry):
            for j in range(level.ny):
                for k in range(2):
                    b[number][i, j, k] = b[number][i, j, k].T
            return carry

        lax.fori_loop(0, level.nz, row, 0)

    if NARROW_SOURCE[0]:
        narrow_own(levels[0], f[0], w[0])
    if NARROW[0]:
        narrow_own(levels[0], u[0], v[0])
    pl.semaphore_wait(barrier, len(partners))
    send("vwuft", 0)
    send_inputs(1)
    for number in range(1, n):
        loads[("l", number)].wait()
        index_lines(number)
    for number in range(n):
        if number:
            loads[("g", number)].wait()
            prolong(number)
            if number == 1:
                send_inputs(3)
                turn(3)
        else:
            turn(1)
        for kind in ("f", "w", "t"):
            receive(kind, number)
        if NARROW_SOURCE[number]:
            widen_far(levels[number], RADIUS - 1, w[number], f[number])
        for kind in ("u", "v"):
            receive(kind, number)
        if NARROW[number]:
            widen_far(levels[number], RADIUS, v[number], u[number])
        smooth(number)
        send("c", number)
        if number == 0:
            send_inputs(2)
            turn(2)
        receive("c", number)
    for group in groups:
        whole(group).wait_send()


def copy_out(*refs):
    results, outs, sem = refs[: len(refs) // 2], refs[len(refs) // 2 : -1], refs[-1]
    copies = [pltpu.make_async_copy(r, o, sem.at[k]) for k, (r, o) in enumerate(zip(results, outs))]
    for copy in copies:
        copy.start()
    for copy in copies:
        copy.wait()


def shards(peers, *arrays):
    fine_to_coarse = lambda group: group[::-1]
    source, guess, shift = (fine_to_coarse(arrays[k : k + 4]) for k in (0, 4, 8))
    blocks, links = (fine_to_coarse(arrays[k : k + 3]) for k in (12, 15))
    n = len(source)
    sides, line = source[0].shape[2:]
    levels, table = plan([x.shape[:2] for x in source], *peers)
    shift = [x.reshape(x.shape[0], x.shape[1], 1, line) for x in shift]
    links = [x if x.shape[1] == x.shape[2] else x.transpose(0, 2, 1) for x in links]
    f32, bf16 = jnp.float32, jnp.bfloat16
    extended = [pltpu.VMEM((l.rows, l.cols, sides, line), f32) for l in levels]
    scratch = extended + extended + [pltpu.VMEM((l.rows, l.cols, 1, line), f32) for l in levels] + extended + extended
    scratch += [pltpu.VMEM(x.shape, f32) for x in guess[1:]]
    scratch += [pltpu.VMEM(x.shape, bf16) for x in blocks]
    scratch += [pltpu.VMEM((l.nz + 2, l.ny + 2, sides, line), bf16) for l in levels[:-1]]
    scratch += [pltpu.SMEM((2 * l.nz * l.ny,), jnp.int32) for l in levels[1:]]
    scratch += [pltpu.SMEM(x.shape, jnp.int32) for x in links]
    scratch += [pltpu.VMEM((l.rows, l.cols, sides, line), bf16) for l in levels] * 2
    scratch += [
        pltpu.VMEM((max(group_lines(table, group) for group in groups_of(table)), 1, line), f32),
        pltpu.SemaphoreType.DMA((3 * n + 3 * (n - 1),)),
        pltpu.SemaphoreType.DMA((len(groups_of(table)),)),
        pltpu.SemaphoreType.DMA((len(groups_of(table)),)),
    ]
    hbm, vmem = pl.BlockSpec(memory_space=pltpu.HBM), pl.BlockSpec(memory_space=pltpu.VMEM)
    operands = [pltpu.with_memory_space_constraint(x, pltpu.HBM) for x in (*source, *guess, *shift, *blocks, *links)]
    shapes = [jax.ShapeDtypeStruct(x.shape, f32) for x in source]
    results = pl.pallas_call(
        functools.partial(kernel, levels, table, peers),
        out_shape=shapes,
        in_specs=[hbm] * len(operands),
        out_specs=[vmem] * n,
        scratch_shapes=scratch,
        compiler_params=pltpu.CompilerParams(
            collective_id=0, has_side_effects=True, vmem_limit_bytes=32 * 1024 * 1024
        ),
    )(*operands)
    results = pl.pallas_call(
        copy_out,
        out_shape=shapes,
        in_specs=[pl.BlockSpec(memory_space=pl.ANY)] * n,
        out_specs=[hbm] * n,
        scratch_shapes=[pltpu.SemaphoreType.DMA((n,))],
        compiler_params=pltpu.CompilerParams(vmem_limit_bytes=2 * 1024 * 1024),
    )(*results)
    return tuple(results[::-1])


def solution(mesh):
    wide = P("gz", "gy", None, None)
    flat = P("gz", "gy", None)
    in_specs = (wide,) * 8 + (flat,) * 4 + (P("gz", "gy", None, None, None),) * 3 + (flat,) * 3
    peers = (mesh.shape["gz"], mesh.shape["gy"])
    return jax.shard_map(
        functools.partial(shards, peers), mesh=mesh, in_specs=in_specs, out_specs=(wide,) * 4, check_vma=False
    )
```

```python
import functools

import jax
import jax.numpy as jnp
from jax import lax
from jax.experimental import pallas as pl
from jax.experimental.pallas import tpu as pltpu
from jax.sharding import PartitionSpec as P

MESH = pl.DeviceIdType.MESH

upper_edge = 14.0
lower_edge = upper_edge / 8.0
CENTRE = (upper_edge + lower_edge) / 2.0
HALF = (upper_edge - lower_edge) / 2.0
RATIO = CENTRE / HALF
FACTOR_0 = 1.0 / RATIO
FACTOR_1 = 1.0 / (2.0 * RATIO - FACTOR_0)
FACTOR_2 = 1.0 / (2.0 * RATIO - FACTOR_1)
A2, B2 = FACTOR_1 * FACTOR_0, 2.0 * FACTOR_1 / HALF
A3, B3 = FACTOR_2 * FACTOR_1, 2.0 * FACTOR_2 / HALF

RADIUS = 3
RINGS = (0, 1, 1, 0)
NARROW = (False, True, True, True)
NARROW_SOURCE = (True, True, True, True)
STRAIGHT = 72
EARLY = (False, False, False, True)
PROLONG_ROWS = 2
PIECE = 2
ROWS = 5


class Level:
    def __init__(self, nz, ny, peers_z, peers_y, ring):
        self.nz, self.ny, self.ring = nz, ny, ring
        self.peers_y = peers_y
        self.halo = RADIUS + ring
        self.total_y = ny * peers_y
        self.full = ny + 2 * self.halo >= self.total_y
        self.rows = nz + 2 * self.halo
        self.cols = self.total_y if self.full else ny + 2 * self.halo
        self.off = 0 if self.full else self.halo

    def col(self, y):
        return y % self.total_y if self.full else y + self.off

    def gap(self, z, y, ring):
        def along(p, n):
            return max(0, -p - ring, p - (n - 1) - ring)

        turns = (-1, 0, 1) if self.full else (0,)
        return along(z, self.nz), min(along(y + t * self.total_y, self.ny) for t in turns)

    def needs(self, z, y, radius, near):
        if sum(self.gap(z, y, self.ring)) > radius:
            return False
        return near is None or near == (max(self.gap(z, y, 0)) == 1)

    def messages(self, radius, near=None):
        found = []
        reach = -(-self.halo // self.nz)
        offsets_y = range(-(self.peers_y // 2 - 1), self.peers_y // 2 + 1) if self.full else range(-1, 2)
        for oz in range(-reach, reach + 1):
            for oy in offsets_y:
                if (oz, oy) == (0, 0):
                    continue
                spans = []
                for i in range(self.nz):
                    js = [j for j in range(self.ny) if self.needs(i - oz * self.nz, j - oy * self.ny, radius, near)]
                    if not js:
                        continue
                    assert js == list(range(js[0], js[-1] + 1))
                    span = (js[0], len(js))
                    if spans and spans[-1][1] == span and spans[-1][0] + spans[-1][2] == i:
                        spans[-1][2] += 1
                    else:
                        spans.append([i, span, 1])
                for i, (j, count), rows in spans:
                    for part in range(i, i + rows, PIECE):
                        found.append((oz, oy, part, j, min(PIECE, i + rows - part), count))
        return sorted(found, key=lambda m: -abs(m[1]))

    def far_cells(self, radius):
        return sorted(
            {
                (self.halo + i + a - oz * self.nz, self.col(j + k - oy * self.ny))
                for oz, oy, i, j, rows, count in self.messages(radius, False)
                for a in range(rows)
                for k in range(count)
            }
        )


def ring_messages(nz, ny):
    found = []
    for oz in (-1, 0, 1):
        for oy in (-1, 0, 1):
            if (oz, oy) == (0, 0):
                continue
            i, rows = (0, nz) if oz == 0 else ((nz - 1, 1) if oz == 1 else (0, 1))
            j, count = (0, ny) if oy == 0 else ((ny - 1, 1) if oy == 1 else (0, 1))
            found.append((oz, oy, i, j, rows, count))
    return found


def plan(shapes, peers_z, peers_y):
    levels = [Level(nz, ny, peers_z, peers_y, ring) for (nz, ny), ring in zip(shapes, RINGS)]
    table = []
    for number, level in enumerate(levels):
        for wide, narrow, radius, split in (("u", "v", RADIUS, NARROW[number]), ("f", "w", RADIUS - 1, NARROW_SOURCE[number])):
            table += [(wide, number, m) for m in level.messages(radius, True if split else None)]
            if split:
                table += [(narrow, number, m) for m in level.messages(radius, False)]
        table += [("t", number, m) for m in level.messages(RADIUS - 1)]
        if number < len(levels) - 1 and level.ring == 0:
            table += [("c", number, m) for m in ring_messages(level.nz, level.ny)]
    return levels, table


def groups_of(table):
    return sorted({(kind, number) for kind, number, _ in table})


def group_lines(table, group):
    lines = {"u": 16, "v": 8, "f": 16, "w": 8, "t": 1, "c": 8}[group[0]]
    return sum(lines * m[4] * m[5] for kind, number, m in table if (kind, number) == group)


def by_way(kind, number, message):
    oz, oy, _, _, rows, count = message
    return (-(abs(oy) + (abs(oz) + 1) // 2), rows * count)


ORDER = by_way


def modulo(value, size):
    return (value + size) & (size - 1) if size & (size - 1) == 0 else lax.rem(value + size, size)


def rolls(v):
    return pltpu.roll(v, 1, 1) + pltpu.roll(v, v.shape[1] - 1, 1)


def kernel(levels, table, peers, *refs):
    n = len(levels)
    source, guess, shift = refs[0:n], refs[n : 2 * n], refs[2 * n : 3 * n]
    refs = refs[3 * n :]
    blocks, links = (None,) + refs[: n - 1], (None,) + refs[n - 1 : 2 * n - 2]
    refs = refs[2 * n - 2 :]
    outs, refs = refs[:n], refs[n:]
    u, f, t, d1, d2 = (refs[k * n : (k + 1) * n] for k in range(5))
    refs = refs[5 * n :]
    g, b, c = (None,) + refs[: n - 1], (None,) + refs[n - 1 : 2 * n - 2], refs[2 * n - 2 : 3 * n - 3]
    lines, link_lines = (None,) + refs[3 * n - 3 : 4 * n - 4], (None,) + refs[4 * n - 4 : 5 * n - 5]
    v, w = refs[5 * n - 5 : 6 * n - 5], refs[6 * n - 5 : 7 * n - 5]
    sizer, local_sem, send_sem, recv_sem = refs[7 * n - 5 :]
    c_flat = [x.reshape((-1,) + x.shape[2:]) for x in c]

    peers_z, peers_y = peers
    my_z, my_y = lax.axis_index("gz"), lax.axis_index("gy")

    def peer(oz, oy):
        return (lax.rem(my_z + (oz + peers_z), peers_z), lax.rem(my_y + (oy + peers_y), peers_y))

    barrier = pltpu.get_barrier_semaphore()
    partners = sorted({m[:2] for _, _, m in table})
    for oz, oy in partners:
        pl.semaphore_signal(barrier, inc=1, device_id=peer(oz, oy), device_id_type=MESH)

    loads = {}

    def load(key, src, dst):
        loads[key] = pltpu.make_async_copy(src, dst, local_sem.at[len(loads)])
        loads[key].start()

    for number, level in enumerate(levels):
        own = (pl.ds(level.halo, level.nz), pl.ds(level.off, level.ny))
        load(("f", number), source[number], f[number].at[own])
        load(("t", number), shift[number], t[number].at[own])
        if number == 0:
            load(("g", 0), guess[0], u[0].at[own])
    for number in range(1, n):
        load(("l", number), links[number], link_lines[number])
        load(("g", number), guess[number], g[number])
        load(("b", number), blocks[number], b[number])

    buffers = {"u": u, "v": v, "f": f, "w": w, "t": t, "c": c}
    groups = groups_of(table)

    def describe(index):
        kind, number, (oz, oy, i, j, rows, count) = table[index]
        level, ref = levels[number], buffers[kind][number]
        zi, yj = i - oz * level.nz, j - oy * level.ny
        if kind == "c":
            source_at = (pl.ds(1 + i, rows), pl.ds(1 + j, count))
            target_at = (pl.ds(1 + zi, rows), pl.ds(1 + yj, count))
        else:
            source_at = (pl.ds(level.halo + i, rows), pl.ds(level.col(j), count))
            target_at = (pl.ds(level.halo + zi, rows), pl.ds(level.col(yj), count))
        return pltpu.make_async_remote_copy(
            src_ref=ref.at[source_at],
            dst_ref=ref.at[target_at],
            send_sem=send_sem.at[groups.index((kind, number))],
            recv_sem=recv_sem.at[groups.index((kind, number))],
            device_id=peer(oz, oy),
            device_id_type=MESH,
        )

    def send(kinds, number, end=None):
        chosen = [
            index
            for index, (k, l, m) in enumerate(table)
            if k in kinds and l == number and (end is None or m[2] + m[4] == end)
        ]
        for index in sorted(chosen, key=lambda index: ORDER(*table[index])):
            describe(index).start()

    def whole(group):
        size, place = group_lines(table, group), groups.index(group)
        every = sizer.at[pl.ds(0, size)]
        return pltpu.make_async_remote_copy(
            every, every, send_sem.at[place], recv_sem.at[place], device_id=peer(0, 1), device_id_type=MESH
        )

    def receive(kind, number):
        if (kind, number) in groups:
            whole((kind, number)).wait_recv()

    def sweep(level, ring, body, rows=None, done=0):
        if done:
            inner = (done, level.nz - done)
            sweep(level, ring, body, (-ring, inner[0]))
            sides = [*range(-ring, done), *range(level.ny - done, level.ny + ring)]
            cells(level, body, inner, [level.col(y) for y in sides])
            sweep(level, ring, body, (inner[1], level.nz + ring))
            return
        cols = sorted({level.col(y) for y in range(-ring, level.ny + ring)})
        cells(level, body, rows or (-ring, level.nz + ring), cols)

    def cells(level, body, rows, cols):
        first, count = level.halo + rows[0], rows[1] - rows[0]
        step = count if count * len(cols) <= STRAIGHT else max(k for k in range(1, ROWS + 1) if count % k == 0)

        def some(start):
            for z in range(step):
                for y in cols:
                    body(start + z, y)

        if step == count:
            some(first)
        else:
            lax.fori_loop(0, count // step, lambda i, carry: (some(first + i * step), carry)[1], 0)

    def beside(level, ref, z, y, middle):
        up, down = ((y + 1) % level.cols, (y - 1) % level.cols) if level.full else (y + 1, y - 1)
        return ref[z - 1, y] + ref[z + 1, y] + ref[z, up] + ref[z, down] + rolls(middle)

    def smooth(number, early=False):
        level = levels[number]
        done = 1 if EARLY[number] else 0
        uu, ff, tt, p, q = u[number], f[number], t[number], d1[number], d2[number]
        ring = level.ring

        def first(z, y):
            v = uu[z, y]
            p[z, y] = (ff[z, y] - ((6.0 + tt[z, y]) * v - beside(level, uu, z, y, v))) * (1.0 / CENTRE)

        def second(z, y):
            v = p[z, y]
            q[z, y] = ((A2 + B2 * CENTRE) - B2 * (6.0 + tt[z, y])) * v + B2 * beside(level, p, z, y, v)

        def third(z, y):
            v, w = q[z, y], p[z, y]
            out = uu[z, y] + (1.0 - B3 * A2 / B2) * w
            out = out + ((1.0 + A3 + B3 / B2) - B3 * (6.0 + tt[z, y])) * v + B3 * beside(level, q, z, y, v)
            finish(z, y, out)

        def finish(z, y, out):
            row, col = z - level.halo, y - level.off
            if ring == 0 or (0 <= row < level.nz and 0 <= col < level.ny):
                outs[number][row, col] = out
            if number < n - 1:
                at = (col + 1) % level.total_y if level.full else col + 1
                c[number][row + 1, at] = out.astype(jnp.bfloat16)

        if early:
            sweep(level, -1, first)
            sweep(level, -2, second)
            return
        sweep(level, ring + 2, first, done=done)
        sweep(level, ring + 1, second, done=2 * done)
        sweep(level, ring, third)

    def index_lines(number):
        level, coarse = levels[number], levels[number - 1]
        base_row = my_z * coarse.nz - 1
        base_col = my_y * coarse.ny - 1

        def row(i, carry):
            for j in range(level.ny):
                for k in range(2):
                    link = link_lines[number][(i, j, k) if level.ny == 2 else (i, k, j)]
                    at_row = modulo(link // coarse.total_y - base_row, coarse.nz * peers_z)
                    at_col = modulo(link - base_col, coarse.total_y)
                    at = jnp.minimum(at_row, coarse.nz + 1) * (coarse.ny + 2) + jnp.minimum(at_col, coarse.ny + 1)
                    lines[number][(i * level.ny + j) * 2 + k] = at
            return carry

        lax.fori_loop(0, level.nz, row, 0)

    def prolong(number):
        level = levels[number]

        def row(i, carry):
            for j in range(level.ny):
                at = (i * level.ny + j) * 2
                picked = [c_flat[number - 1][lines[number][at + k]] for k in range(2)]
                total = g[number][i, j] + lax.dot_general(
                    jnp.concatenate(picked, axis=1),
                    jnp.concatenate([b[number][i, j, 0], b[number][i, j, 1]], axis=0),
                    (((1,), (0,)), ((), ())),
                    preferred_element_type=jnp.float32,
                )
                u[number][level.halo + i, level.off + j] = total
                if NARROW[number]:
                    v[number][level.halo + i, level.off + j] = total.astype(jnp.bfloat16)
            return carry

        ends = sorted({m[2] + m[4] for k, l, m in table if l == number and k in ("u", "v")} | {level.nz})
        start = 0
        for end in ends:
            step = max(k for k in range(1, PROLONG_ROWS + 1) if (end - start) % k == 0)

            def some(i, carry, start=start, step=step):
                for k in range(step):
                    row(start + i * step + k, carry)
                return carry

            lax.fori_loop(0, (end - start) // step, some, 0)
            send("uv", number, end)
            start = end

    for key in (("f", 0), ("t", 0), ("g", 0)):
        loads[key].wait()
    def narrow_own(level, wide, narrow):
        def row(i, carry):
            for j in range(level.ny):
                narrow[level.halo + i, level.off + j] = wide[level.halo + i, level.off + j].astype(jnp.bfloat16)
            return carry

        lax.fori_loop(0, level.nz, row, 0)

    def widen_far(level, radius, narrow, wide):
        for z, y in level.far_cells(radius):
            wide[z, y] = narrow[z, y].astype(jnp.float32)

    def send_inputs(number):
        for kind in ("t", "f"):
            loads[(kind, number)].wait()
        if NARROW_SOURCE[number]:
            narrow_own(levels[number], f[number], w[number])
        send("twf", number)

    def turn(number):
        loads[("b", number)].wait()
        level = levels[number]

        def row(i, carry):
            for j in range(level.ny):
                for k in range(2):
                    b[number][i, j, k] = b[number][i, j, k].T
            return carry

        lax.fori_loop(0, level.nz, row, 0)

    if NARROW_SOURCE[0]:
        narrow_own(levels[0], f[0], w[0])
    if NARROW[0]:
        narrow_own(levels[0], u[0], v[0])
    pl.semaphore_wait(barrier, len(partners))
    send("vwuft", 0)
    send_inputs(1)
    for number in range(1, n):
        loads[("l", number)].wait()
        index_lines(number)
    for number in range(n):
        if number:
            loads[("g", number)].wait()
            prolong(number)
            if number == 1:
                send_inputs(3)
                turn(3)
        else:
            turn(1)
        for kind in ("f", "w", "t"):
            receive(kind, number)
        if NARROW_SOURCE[number]:
            widen_far(levels[number], RADIUS - 1, w[number], f[number])
        if EARLY[number]:
            smooth(number, early=True)
        for kind in ("u", "v"):
            receive(kind, number)
        if NARROW[number]:
            widen_far(levels[number], RADIUS, v[number], u[number])
        smooth(number)
        send("c", number)
        if number == 0:
            send_inputs(2)
            turn(2)
        receive("c", number)
    for group in groups:
        whole(group).wait_send()


def copy_out(*refs):
    results, outs, sem = refs[: len(refs) // 2], refs[len(refs) // 2 : -1], refs[-1]
    copies = [pltpu.make_async_copy(r, o, sem.at[k]) for k, (r, o) in enumerate(zip(results, outs))]
    for copy in copies:
        copy.start()
    for copy in copies:
        copy.wait()


def shards(peers, *arrays):
    fine_to_coarse = lambda group: group[::-1]
    source, guess, shift = (fine_to_coarse(arrays[k : k + 4]) for k in (0, 4, 8))
    blocks, links = (fine_to_coarse(arrays[k : k + 3]) for k in (12, 15))
    n = len(source)
    sides, line = source[0].shape[2:]
    levels, table = plan([x.shape[:2] for x in source], *peers)
    shift = [x.reshape(x.shape[0], x.shape[1], 1, line) for x in shift]
    links = [x if x.shape[1] == x.shape[2] else x.transpose(0, 2, 1) for x in links]
    f32, bf16 = jnp.float32, jnp.bfloat16
    extended = [pltpu.VMEM((l.rows, l.cols, sides, line), f32) for l in levels]
    scratch = extended + extended + [pltpu.VMEM((l.rows, l.cols, 1, line), f32) for l in levels] + extended + extended
    scratch += [pltpu.VMEM(x.shape, f32) for x in guess[1:]]
    scratch += [pltpu.VMEM(x.shape, bf16) for x in blocks]
    scratch += [pltpu.VMEM((l.nz + 2, l.ny + 2, sides, line), bf16) for l in levels[:-1]]
    scratch += [pltpu.SMEM((2 * l.nz * l.ny,), jnp.int32) for l in levels[1:]]
    scratch += [pltpu.SMEM(x.shape, jnp.int32) for x in links]
    scratch += [pltpu.VMEM((l.rows, l.cols, sides, line), bf16) for l in levels] * 2
    scratch += [
        pltpu.VMEM((max(group_lines(table, group) for group in groups_of(table)), 1, line), f32),
        pltpu.SemaphoreType.DMA((3 * n + 3 * (n - 1),)),
        pltpu.SemaphoreType.DMA((len(groups_of(table)),)),
        pltpu.SemaphoreType.DMA((len(groups_of(table)),)),
    ]
    hbm, vmem = pl.BlockSpec(memory_space=pltpu.HBM), pl.BlockSpec(memory_space=pltpu.VMEM)
    operands = [pltpu.with_memory_space_constraint(x, pltpu.HBM) for x in (*source, *guess, *shift, *blocks, *links)]
    shapes = [jax.ShapeDtypeStruct(x.shape, f32) for x in source]
    results = pl.pallas_call(
        functools.partial(kernel, levels, table, peers),
        out_shape=shapes,
        in_specs=[hbm] * len(operands),
        out_specs=[vmem] * n,
        scratch_shapes=scratch,
        compiler_params=pltpu.CompilerParams(
            collective_id=0, has_side_effects=True, vmem_limit_bytes=32 * 1024 * 1024
        ),
    )(*operands)
    results = pl.pallas_call(
        copy_out,
        out_shape=shapes,
        in_specs=[pl.BlockSpec(memory_space=pl.ANY)] * n,
        out_specs=[hbm] * n,
        scratch_shapes=[pltpu.SemaphoreType.DMA((n,))],
        compiler_params=pltpu.CompilerParams(vmem_limit_bytes=2 * 1024 * 1024),
    )(*results)
    return tuple(results[::-1])


def solution(mesh):
    wide = P("gz", "gy", None, None)
    flat = P("gz", "gy", None)
    in_specs = (wide,) * 8 + (flat,) * 4 + (P("gz", "gy", None, None, None),) * 3 + (flat,) * 3
    peers = (mesh.shape["gz"], mesh.shape["gy"])
    return jax.shard_map(
        functools.partial(shards, peers), mesh=mesh, in_specs=in_specs, out_specs=(wide,) * 4, check_vma=False
    )
```
